256 devices in a mesh: dp: 8 (over y, core), tensor: 4 (over x), ctx: 8 (over z).
Axes of the slice: x: 4, y: 4, z: 8, core: 2. Of those that a mesh axis runs over, the one named last changes fastest.
Arguments:
- grad_down: bfloat16 [8, 18432, 4608], P('dp', 'tensor', 'ctx'), may hold values from -700 to 700
- grad_query: bfloat16 [8, 4608, 2048], P('dp', 'ctx', 'tensor'), may hold values from -700 to 700
- down_param: float32 [18432, 4608], P(('tensor', 'dp'), 'ctx'), may hold values from -0.3 to 0.3
- down_moment: float32 [18432, 4608], P(('tensor', 'dp'), 'ctx'), may hold values from -6 to 6
- down_second: float32 [4608], P('ctx'), may hold values from 0.1 to 2
- query_param: float32 [4608, 2048], P(('ctx', 'dp'), 'tensor'), may hold values from -0.3 to 0.3
- query_moment: float32 [4608, 2048], P(('ctx', 'dp'), 'tensor'), may hold values from -6 to 6
- query_second: float32 [16], P('tensor'), may hold values from 0.1 to 2
- step_count: int32 [1], replicated, may hold values from 1 to 29
Outputs:
- down_param_new: float32 [18432, 4608], P(('tensor', 'dp'), 'ctx')
- down_moment_new: float32 [18432, 4608], P(('tensor', 'dp'), 'ctx')
- down_second_new: float32 [4608], P('ctx')
- down_update: bfloat16 [18432, 4608], P(('tensor', 'dp'), 'ctx')
- query_param_new: float32 [4608, 2048], P(('ctx', 'dp'), 'tensor')
- query_moment_new: float32 [4608, 2048], P(('ctx', 'dp'), 'tensor')
- query_second_new: float32 [16], P('tensor')
- query_update: bfloat16 [4608, 2048], P(('ctx', 'dp'), 'tensor')
The draws below stay inside these ranges and needn't reach their ends.
All inputs are finite; a program needn't handle non-finite values.
Results may differ from the reference program's by a relative error of at most 0.012.
Values may be sent and summed in bfloat16 or wider, within the bound.
A program may use at most 64 MiB of HBM per device.

```python
import math
import jax
import jax.numpy as jnp
from jax import lax

D = 4608
HEAD_DIM = 128
FF = 18432
HEADS = 16
N_DP = 8


def gradient_field(key, row_count, col_count):
    subkeys = jax.random.split(key, 4)
    row_ramp = jnp.sqrt(3.0) ** (jnp.arange(row_count, dtype=jnp.float32) / row_count)
    row_scale = jnp.exp(jax.random.uniform(subkeys[0], (row_count,), jnp.float32, 0.0, math.log(10.0))) * row_ramp
    col_spread = math.log(10.0)
    col_scale = jnp.exp(jax.random.uniform(subkeys[1], (col_count,), jnp.float32, 0.0, col_spread))
    replica_ramp = jnp.sqrt(3.0) ** (jnp.arange(N_DP, dtype=jnp.float32) / max(N_DP - 1, 1))
    entries = 0.1 * math.sqrt(N_DP) * jax.random.truncated_normal(subkeys[3], -4.0, 4.0, (N_DP, row_count, col_count), jnp.float32)
    return entries * replica_ramp[:, None, None] * row_scale[None, :, None] * col_scale[None, None, :]


def draw_grad_down(key, part):
    return gradient_field(jax.random.fold_in(key, 11), FF, D).astype(jnp.bfloat16)


def draw_grad_query(key, part):
    return gradient_field(jax.random.fold_in(key, 23), D, HEADS * HEAD_DIM).astype(jnp.bfloat16)


def block_levels(key, extent, shards, least, largest):
    def one(axis_at, blocks):
        heights = jax.random.uniform(jax.random.fold_in(jax.random.fold_in(key, 6), axis_at), (blocks,), jnp.float32, least / len(shards), largest / len(shards))
        return jnp.repeat(jnp.exp(heights), extent[axis_at] // blocks).reshape((-1,) + (1,) * (len(extent) - axis_at - 1))

    loudness = one(*shards[0])
    for cut in shards[1:]:
        loudness = loudness * one(*cut)
    return loudness


def gaussian(rng, extent, width, limit, pieces=(), kind=jnp.bfloat16):
    gain = block_levels(rng, extent, pieces, -0.22, 0.18) if pieces else 1.0
    result = jax.random.normal(rng, extent, jnp.float32) * width * gain
    return jnp.minimum(jnp.maximum(result, -limit), limit).astype(kind)


def setup_inputs(seed: int = 0) -> dict:
    keys = jax.random.split(jax.random.key(seed), 10)
    grad_down = draw_grad_down(jax.random.fold_in(keys[9], 71), 0)
    grad_query = draw_grad_query(jax.random.fold_in(keys[9], 71), 0)
    down_param = gaussian(keys[2], (FF, D), 0.05, 0.3, ((0, 32), (1, 8)), jnp.float32)
    down_moment = gaussian(keys[3], (FF, D), 1.0, 6.0, ((0, 32), (1, 8)), jnp.float32)
    down_second = jnp.clip(jnp.exp(math.log(2.0) - 2.9957323 * jax.random.uniform(keys[4], (D,), jnp.float32) ** block_levels(keys[4], (D,), ((0, 8),), -0.2, 0.2)), 0.1, 2.0)
    query_param = gaussian(keys[5], (D, HEADS * HEAD_DIM), 0.05, 0.3, ((0, 64), (1, 4)), jnp.float32)
    query_moment = gaussian(keys[6], (D, HEADS * HEAD_DIM), 1.0, 6.0, ((0, 64), (1, 4)), jnp.float32)
    query_second = jnp.clip(jnp.exp(math.log(2.0) - 2.9957323 * jax.random.uniform(keys[7], (HEADS,), jnp.float32) ** block_levels(keys[7], (HEADS,), ((0, 4),), -0.2, 0.2)), 0.1, 2.0)
    step_count = jax.random.randint(keys[8], (1,), 1, 30).astype(jnp.int32)
    return dict(grad_down=grad_down, grad_query=grad_query, down_param=down_param, down_moment=down_moment, down_second=down_second, query_param=query_param, query_moment=query_moment, query_second=query_second, step_count=step_count)


BETA_ONE = 0.9
BETA_TWO = 0.95
EPSILON = 1e-08
LEARN_RATE = 0.003
DECAY_RATE = 0.1

def replica_mean(gradients):

    def accumulate(position, running_total):
        return running_total + lax.dynamic_index_in_dim(gradients, position, 0, keepdims=False).astype(jnp.float32)
    summed = lax.fori_loop(0, gradients.shape[0], accumulate, jnp.zeros(gradients.shape[1:], jnp.float32))
    return summed / gradients.shape[0]

def finish(parameter, moment, gradient, second_wide, keep_one, keep_two):
    moment_new = BETA_ONE * moment + (1.0 - BETA_ONE) * gradient
    update = moment_new / keep_one / (jnp.sqrt(second_wide / keep_two) + EPSILON)
    parameter_new = parameter - LEARN_RATE * (update + DECAY_RATE * parameter)
    return (parameter_new, moment_new, update.astype(jnp.bfloat16))

def reference(grad_down, grad_query, down_param, down_moment, down_second, query_param, query_moment, query_second, step_count):
    step_value = step_count[0].astype(jnp.float32)
    keep_one = 1.0 - jnp.power(jnp.float32(BETA_ONE), step_value)
    keep_two = 1.0 - jnp.power(jnp.float32(BETA_TWO), step_value)
    down_grad = replica_mean(grad_down)
    query_grad = replica_mean(grad_query)
    neuron_mean = lax.optimization_barrier(jnp.sum(down_grad * down_grad, axis=0)) / FF
    head_mean = lax.optimization_barrier(jnp.sum((query_grad * query_grad).reshape(D, HEADS, HEAD_DIM), axis=(0, 2))) / (D * HEAD_DIM)
    down_second_new = BETA_TWO * down_second + (1.0 - BETA_TWO) * neuron_mean
    query_second_new = BETA_TWO * query_second + (1.0 - BETA_TWO) * head_mean
    down_param_new, down_moment_new, down_update = finish(down_param, down_moment, down_grad, down_second_new[None, :], keep_one, keep_two)
    query_wide = jnp.repeat(query_second_new, HEAD_DIM)
    query_param_new, query_moment_new, query_update = finish(query_param, query_moment, query_grad, query_wide[None, :], keep_one, keep_two)
    return (down_param_new, down_moment_new, down_second_new, down_update, query_param_new, query_moment_new, query_second_new, query_update)
```

```python
import functools
import math

import jax
import jax.numpy as jnp
from jax import lax
from jax.experimental import pallas as pl
from jax.experimental.pallas import tpu as pltpu
from jax.sharding import PartitionSpec as P

D = 4608
HEAD_DIM = 128
FF = 18432

BETA_ONE = 0.9
BETA_TWO = 0.95
EPSILON = 1e-08
LEARN_RATE = 0.003
DECAY_RATE = 0.1

MESH = pl.DeviceIdType.MESH
F32 = jnp.float32
BF16 = jnp.bfloat16

FAR, RIGHT, LEFT, SELF = range(4)
PLUS, MINUS = range(2)
LANES = 128
TILES = 4


def exchange(
    gd, gq, steps, dsec, qsec,
    g_out, t_out, q_out, n_out,
    own_d, prt_d, own_t, prt_t, own_q, prt_q,
    snd_a, snd_b, snd_t, snd_q, rly_a, rly_b, rly_t, rly_q,
    fin_pa, fin_pb, fin_ma, fin_mb, fin_tp, fin_tm, fin_q,
    tbuf, zbuf, dbuf, xbuf, dsec_v, qsec_v,
    own_sem, ds_sem, dr_sem, ss, rs_rly, rs_fin, tsem, zs, zr, ps, pr, xs, xr, small_sem,
):
    dp, tp, cp = lax.axis_index("dp"), lax.axis_index("tensor"), lax.axis_index("ctx")
    y, core = dp // 2, dp % 2
    nz = zbuf.shape[0]
    cols_all, wide = own_d.shape[1], own_d.shape[2]
    cut = 2 * LANES
    rest = cols_all - cut
    t_cols = cols_all // 2
    pair = 2 * wide + LANES
    rows_q, q_cols = own_q.shape[1], own_q.shape[2]
    q_half = q_cols // 2
    at = {FAR: (y + 2) % 4, RIGHT: (y + 1) % 4, LEFT: (y + 3) % 4, SELF: y}
    partner = y * 2 + (1 - core)

    span = {"A": (0, cut), "B": (cut, rest), "AB": (0, cols_all)}

    def main_piece(role, who, part, first, tiles):
        row, count = span[part]
        lanes = pl.multiple_of(at[role] * pair + who * (wide + LANES) + first * LANES, LANES)
        return gd.at[0, pl.ds(row, count), pl.ds(lanes, tiles * LANES)]

    def tile_piece(role, who):
        lanes = pl.multiple_of(at[role] * pair + wide, LANES)
        return gd.at[0, pl.ds(pl.multiple_of(who * t_cols, 16), t_cols), pl.ds(lanes, LANES)]

    def query_piece(role, who):
        return gq.at[0, pl.ds(pl.multiple_of((at[role] * 2 + who) * rows_q, 8), rows_q), :]

    order = [("q", FAR), ("t", FAR)] + [("d", FAR, "AB", k, 1) for k in range(TILES)]
    order += [("q", RIGHT), ("q", LEFT), ("d", RIGHT, "B", 0, TILES), ("t", LEFT), ("d", LEFT, "A", 0, TILES)]
    order += [("t", RIGHT), ("d", RIGHT, "A", 0, TILES), ("d", LEFT, "B", 0, TILES)]
    order += [("q", SELF), ("t", SELF), ("d", SELF, "AB", 0, TILES)]

    def piece(item, who):
        if item[0] == "q":
            return query_piece(item[1], who)
        if item[0] == "t":
            return tile_piece(item[1], who)
        return main_piece(item[1], who, *item[2:])

    def landing(item, d, t, q):
        if item[0] == "q":
            return q.at[item[1]]
        if item[0] == "t":
            return t.at[item[1]]
        _, role, part, first, tiles = item
        row, count = span[part]
        return d.at[role, pl.ds(row, count), pl.ds(first * LANES, tiles * LANES)]

    own_copy = [
        pltpu.make_async_copy(piece(item, core), landing(item, own_d, own_t, own_q), own_sem.at[n])
        for n, item in enumerate(order)
    ]
    for copy in own_copy:
        copy.start()

    barrier = pltpu.get_barrier_semaphore()
    greeted = 0
    for k in range(1, 8):
        pl.semaphore_signal(barrier, inc=1, device_id=((dp + k) % 8, tp, cp), device_id_type=MESH)
        greeted += 1
    for k in range(1, 4):
        pl.semaphore_signal(barrier, inc=1, device_id=(dp, (tp + k) % 4, cp), device_id_type=MESH)
        greeted += 1
    for k in (1, nz - 1):
        pl.semaphore_signal(barrier, inc=1, device_id=(dp, tp, (cp + k) % nz), device_id_type=MESH)
        greeted += 1
    pl.semaphore_wait(barrier, greeted)

    prt_copy = [
        pltpu.make_async_remote_copy(
            src_ref=piece(item, 1 - core), dst_ref=landing(item, prt_d, prt_t, prt_q),
            send_sem=ds_sem.at[n], recv_sem=dr_sem.at[n],
            device_id=(partner, tp, cp), device_id_type=MESH)
        for n, item in enumerate(order)
    ]
    for copy in prt_copy:
        copy.start()

    small = [
        pltpu.make_async_copy(dsec, dsec_v, small_sem.at[1]),
        pltpu.make_async_copy(qsec, qsec_v, small_sem.at[2]),
    ]
    for copy in small:
        copy.start()

    have = set()

    def need(test):
        for n, item in enumerate(order):
            if n not in have and test(item):
                have.add(n)
                own_copy[n].wait()
                prt_copy[n].wait_recv()

    def main_sum(role, part, k):
        need(lambda item: item[0] == "d" and item[1] == role and part in item[2] and item[3] <= k < item[3] + item[4])
        row, count = span[part]
        here = (role, pl.ds(row, count), pl.ds(k * LANES, LANES))
        return own_d[here].astype(F32) + prt_d[here].astype(F32)

    def tile_sum(role):
        need(lambda item: item == ("t", role))
        return own_t[role].astype(F32) + prt_t[role].astype(F32)

    def query_sum(role, block):
        need(lambda item: item == ("q", role))
        here = (role, slice(None), pl.ds(block * q_half, q_half))
        return own_q[here].astype(F32) + prt_q[here].astype(F32)

    y_copies = []
    counters = {"s": 0, "r": 0, "f": 0}

    def y_send(direction, src, dst, landing_sems, kind):
        target = at[RIGHT] if direction == PLUS else at[LEFT]
        s, r = counters["s"], counters[kind]
        counters["s"] += 1
        counters[kind] += 1
        copy = pltpu.make_async_remote_copy(
            src_ref=src, dst_ref=dst, send_sem=ss.at[s], recv_sem=landing_sems.at[r],
            device_id=(target * 2 + core, tp, cp), device_id_type=MESH)
        copy.start()
        y_copies.append(copy)
        return copy

    relayed, plain, joined = {}, {}, {}

    def store_send(direction, value, src, dst, landing_sems, kind):
        src[...] = value.astype(BF16)
        return y_send(direction, src, dst, landing_sems, kind)

    def first_q():
        for way in (PLUS, MINUS):
            relayed[way, "q"] = store_send(way, query_sum(FAR, way), snd_q.at[way, 0], rly_q.at[way], rs_rly, "r")

    def second_q():
        for way, role in ((PLUS, RIGHT), (MINUS, LEFT)):
            plain[way, "q"] = store_send(way, query_sum(role, 1 - way), snd_q.at[way, 1], fin_q.at[way, 0], rs_fin, "f")

    def third_q():
        for way, role in ((PLUS, RIGHT), (MINUS, LEFT)):
            relayed[way, "q"].wait_recv()
            value = query_sum(role, way) + rly_q[way].astype(F32)
            joined[way, "q"] = store_send(way, value, snd_q.at[way, 2], fin_q.at[way, 1], rs_fin, "f")

    def first_t():
        relayed["t"] = store_send(PLUS, tile_sum(FAR), snd_t.at[0], rly_t, rs_rly, "r")

    def second_t():
        plain["t"] = store_send(MINUS, tile_sum(LEFT), snd_t.at[1], fin_tm, rs_fin, "f")

    def third_t():
        relayed["t"].wait_recv()
        value = tile_sum(RIGHT) + rly_t[...].astype(F32)
        joined["t"] = store_send(PLUS, value, snd_t.at[2], fin_tp, rs_fin, "f")

    def first_d(k):
        relayed[PLUS, k] = store_send(PLUS, main_sum(FAR, "A", k), snd_a.at[0, k], rly_a.at[k], rs_rly, "r")
        relayed[MINUS, k] = store_send(MINUS, main_sum(FAR, "B", k), snd_b.at[0, k], rly_b.at[k], rs_rly, "r")

    def second_d(k):
        plain[PLUS, k] = store_send(PLUS, main_sum(RIGHT, "B", k), snd_b.at[1, k], fin_pb.at[k], rs_fin, "f")
        plain[MINUS, k] = store_send(MINUS, main_sum(LEFT, "A", k), snd_a.at[1, k], fin_ma.at[k], rs_fin, "f")

    def third_d(k):
        relayed[PLUS, k].wait_recv()
        value = main_sum(RIGHT, "A", k) + rly_a[k].astype(F32)
        joined[PLUS, k] = store_send(PLUS, value, snd_a.at[2, k], fin_pa.at[k], rs_fin, "f")
        relayed[MINUS, k].wait_recv()
        value = main_sum(LEFT, "B", k) + rly_b[k].astype(F32)
        joined[MINUS, k] = store_send(MINUS, value, snd_b.at[2, k], fin_mb.at[k], rs_fin, "f")

    first_q()
    first_t()
    first_d(0)
    second_q()
    first_d(1)
    third_q()
    first_d(2)
    first_d(3)
    second_t()
    for k in range(TILES):
        second_d(k)
    third_t()
    for k in range(TILES):
        third_d(k)

    head_row = jnp.zeros((1, LANES), F32)
    lane = lax.broadcasted_iota(jnp.int32, (1, LANES), 1)
    for block in (0, 1):
        joined[block, "q"].wait_recv()
        plain[1 - block, "q"].wait_recv()
        mean = (query_sum(SELF, block) + fin_q[block, 1].astype(F32) + fin_q[1 - block, 0].astype(F32)) / 8
        q_out[:, pl.ds(block * q_half, q_half)] = mean
        square = jnp.sum(mean * mean, axis=0, keepdims=True)
        for h in range(2):
            part = jnp.sum(square[:, h * LANES:(h + 1) * LANES], axis=1, keepdims=True)
            head_row = jnp.where(lane == block * 2 + h, part, head_row)
    zbuf[cp] = jnp.broadcast_to(head_row, (8, LANES))

    ring, z_copies = {}, []
    for s in range(nz // 2):
        for way, count in ((PLUS, nz // 2), (MINUS, nz - 1 - nz // 2)):
            if s < count:
                if s > 0:
                    ring[way, s - 1].wait_recv()
                owner = (cp + (nz - s if way == PLUS else s)) % nz
                ring[way, s] = pltpu.make_async_remote_copy(
                    src_ref=zbuf.at[owner], dst_ref=zbuf.at[owner],
                    send_sem=zs.at[way, s], recv_sem=zr.at[way, s],
                    device_id=(dp, tp, (cp + (1 if way == PLUS else nz - 1)) % nz), device_id_type=MESH)
                ring[way, s].start()
                z_copies.append(ring[way, s])
    ring[PLUS, nz // 2 - 1].wait_recv()
    ring[MINUS, nz - 2 - nz // 2].wait_recv()
    head_sum = zbuf[0, pl.ds(0, 1), :]
    for z in range(1, nz):
        head_sum = head_sum + zbuf[z, pl.ds(0, 1), :]

    joined["t"].wait_recv()
    plain["t"].wait_recv()
    mine = pl.ds(pl.multiple_of(core * t_cols, 8), t_cols)
    tbuf[mine, :] = (tile_sum(SELF) + fin_tp[...].astype(F32) + fin_tm[...].astype(F32)) / 8
    swap = pltpu.make_async_remote_copy(
        src_ref=tbuf.at[mine, :], dst_ref=tbuf.at[mine, :], send_sem=tsem.at[0], recv_sem=tsem.at[1],
        device_id=(partner, tp, cp), device_id_type=MESH)
    swap.start()

    def column_squares(rows):
        return jnp.sum(rows * rows, axis=0, keepdims=True)

    sums_a, sums_b = jnp.zeros((1, cut), F32), jnp.zeros((1, rest), F32)
    for k in range(TILES):
        if k == 1:
            swap.wait_recv()
            both = jnp.transpose(tbuf[...])
            own_rows = jnp.where(core == 0, both[:LANES // 2], both[LANES // 2:])
            t_out[...] = own_rows
            sums_a = sums_a + column_squares(own_rows[:, :cut])
            sums_b = sums_b + column_squares(own_rows[:, cut:])
        plain[MINUS, k].wait_recv()
        joined[PLUS, k].wait_recv()
        mean = (main_sum(SELF, "A", k) + fin_pa[k].astype(F32) + fin_ma[k].astype(F32)) / 8
        rows = jnp.transpose(mean)
        g_out[k, :, pl.ds(0, cut)] = rows
        sums_a = sums_a + column_squares(rows)
        plain[PLUS, k].wait_recv()
        joined[MINUS, k].wait_recv()
        mean = (main_sum(SELF, "B", k) + fin_mb[k].astype(F32) + fin_pb[k].astype(F32)) / 8
        rows = jnp.transpose(mean)
        g_out[k, :, pl.ds(cut, rest)] = rows
        sums_b = sums_b + column_squares(rows)

    dbuf[dp] = jnp.zeros((8, LANES), F32)
    dbuf[dp, pl.ds(0, 1), :] = sums_a[:, :LANES]
    dbuf[dp, pl.ds(1, 1), :] = sums_a[:, LANES:]
    dbuf[dp, pl.ds(2, 1), :] = sums_b[:, :LANES]
    dbuf[dp, pl.ds(3, 1), :] = sums_b[:, LANES:2 * LANES]
    dbuf[dp, pl.ds(4, 1), pl.ds(0, LANES // 2)] = sums_b[:, 2 * LANES:]
    dbuf[dp, pl.ds(5, 1), :] = head_sum

    def to_all(buf, me, size, device, send, recv):
        sends = []
        for k in range(1, size):
            copy = pltpu.make_async_remote_copy(
                src_ref=buf.at[me], dst_ref=buf.at[me], send_sem=send.at[k], recv_sem=recv.at[me],
                device_id=device((me + k) % size), device_id_type=MESH)
            copy.start()
            sends.append(copy)
        for k in range(1, size):
            other = (me + k) % size
            pltpu.make_async_remote_copy(
                src_ref=buf.at[other], dst_ref=buf.at[other], send_sem=send.at[k], recv_sem=recv.at[other],
                device_id=device(other), device_id_type=MESH).wait_recv()
        total = buf[0]
        for p in range(1, size):
            total = total + buf[p]
        return total, sends

    for copy in small:
        copy.wait()
    step = jnp.full((1, LANES), steps[0], jnp.int32).astype(F32)
    keep_one = 1.0 - jnp.exp(step * math.log(BETA_ONE))
    keep_two = 1.0 - jnp.exp(step * math.log(BETA_TWO))

    part, p_copies = to_all(dbuf, dp, 8, lambda p: (p, tp, cp), ps, pr)
    xbuf[tp] = part
    whole, x_copies = to_all(xbuf, tp, 4, lambda t: (dp, t, cp), xs, xr)

    def advance(old, mean, n):
        new = BETA_TWO * old + (1.0 - BETA_TWO) * mean
        n_out[n:n + 1, :] = 1.0 / (keep_one * (jnp.sqrt(new / keep_two) + EPSILON))
        n_out[n + 8:n + 9, :] = new

    n_out[...] = jnp.zeros(n_out.shape, F32)
    for k in range(5):
        if k < 4:
            old = dsec_v[pl.ds(k * LANES, LANES)].reshape(1, LANES)
        else:
            old = dsec_v[pl.ds(k * LANES, LANES // 2)].reshape(1, LANES // 2)
            old = jnp.concatenate([old, jnp.ones((1, LANES // 2), F32)], axis=1)
        advance(old, whole[k:k + 1, :] / FF, k)
    old = jnp.ones((1, LANES), F32)
    for h in range(4):
        old = jnp.where(lane == h, qsec_v[h], old)
    advance(old, part[5:6, :] / (D * HEAD_DIM), 5)

    for copy in prt_copy + y_copies + z_copies + [swap] + p_copies + x_copies:
        copy.wait_send()


def finish(
    n_in, g_in, t_in, q_in, dp_in, dm_in, qp_in, qm_in,
    dp_out, dm_out, ds_out, du_out, qp_out, qm_out, qs_out, qu_out,
    po_buf, mo_buf, uo_buf, qpo, qmo, quo, out_sem,
):
    core = lax.axis_index("dp") % 2
    width = dp_in.shape[1]
    half = LANES // 2
    stores = []

    def store(src, dst):
        copy = pltpu.make_async_copy(src, dst, out_sem.at[len(stores)])
        copy.start()
        stores.append(copy)

    def update(param, moment, grad, scale):
        moment_new = BETA_ONE * moment + (1.0 - BETA_ONE) * grad
        step = moment_new * scale
        param_new = param - LEARN_RATE * (step + DECAY_RATE * param)
        return param_new, moment_new, step.astype(BF16)

    def down(grad, first, count):
        rows = pl.ds(pl.multiple_of(first, half), count)
        for k in range(5):
            lanes = pl.ds(k * LANES, LANES if k < 4 else width - 4 * LANES)
            scale = n_in[k:k + 1, :lanes.size]
            po_buf[rows, lanes], mo_buf[rows, lanes], uo_buf[rows, lanes] = update(
                dp_in[rows, lanes], dm_in[rows, lanes], grad[:, lanes], scale)
        store(po_buf.at[rows, :], dp_out.at[rows, :])
        store(mo_buf.at[rows, :], dm_out.at[rows, :])
        store(uo_buf.at[rows, :], du_out.at[rows, :])

    for k in range(TILES):
        down(g_in.at[k], core * half + k * LANES, LANES)
    down(t_in, (1 - core) * TILES * LANES, half)
    for h in range(4):
        lanes = pl.ds(h * LANES, LANES)
        qpo[:, lanes], qmo[:, lanes], quo[:, lanes] = update(
            qp_in[:, lanes], qm_in[:, lanes], q_in[:, lanes], n_in[5:6, h:h + 1])
    store(qpo, qp_out)
    store(qmo, qm_out)
    store(quo, qu_out)
    for k in range(5):
        count = LANES if k < 4 else width - 4 * LANES
        ds_out[pl.ds(k * LANES, count)] = n_in[8 + k:9 + k, :count].reshape(count)
    qs_out[...] = n_in[13:14, :4].reshape(4)
    for copy in stores:
        copy.wait()


def shards(nz, grad_down, grad_query, down_param, down_moment, down_second,
           query_param, query_moment, query_second, step_count):
    rows_d, width = down_param.shape
    rows_q, q_width = query_param.shape
    cut, wide = 2 * LANES, TILES * LANES
    rest, t_cols, q_half = width - cut, width // 2, q_width // 2
    hbm = pl.BlockSpec(memory_space=pltpu.HBM)
    vmem = pl.BlockSpec(memory_space=pltpu.VMEM)
    dma = pltpu.SemaphoreType.DMA
    pieces = 17
    grad_rows = jnp.swapaxes(grad_down, 1, 2)
    in_hbm = lambda x: pltpu.with_memory_space_constraint(x, pltpu.HBM)
    g, t, q, n = pl.pallas_call(
        exchange,
        name="exchange",
        out_shape=(
            jax.ShapeDtypeStruct((TILES, LANES, width), F32),
            jax.ShapeDtypeStruct((LANES // 2, width), F32),
            jax.ShapeDtypeStruct((rows_q, q_width), F32),
            jax.ShapeDtypeStruct((16, LANES), F32),
        ),
        in_specs=[hbm, hbm, pl.BlockSpec(memory_space=pltpu.SMEM), hbm, hbm],
        out_specs=(vmem,) * 4,
        scratch_shapes=[
            pltpu.VMEM((4, width, wide), BF16),
            pltpu.VMEM((4, width, wide), BF16),
            pltpu.VMEM((4, t_cols, LANES), BF16),
            pltpu.VMEM((4, t_cols, LANES), BF16),
            pltpu.VMEM((4, rows_q, q_width), BF16),
            pltpu.VMEM((4, rows_q, q_width), BF16),
            pltpu.VMEM((3, TILES, cut, LANES), BF16),
            pltpu.VMEM((3, TILES, rest, LANES), BF16),
            pltpu.VMEM((3, t_cols, LANES), BF16),
            pltpu.VMEM((2, 3, rows_q, q_half), BF16),
            pltpu.VMEM((TILES, cut, LANES), BF16),
            pltpu.VMEM((TILES, rest, LANES), BF16),
            pltpu.VMEM((t_cols, LANES), BF16),
            pltpu.VMEM((2, rows_q, q_half), BF16),
            pltpu.VMEM((TILES, cut, LANES), BF16),
            pltpu.VMEM((TILES, rest, LANES), BF16),
            pltpu.VMEM((TILES, cut, LANES), BF16),
            pltpu.VMEM((TILES, rest, LANES), BF16),
            pltpu.VMEM((t_cols, LANES), BF16),
            pltpu.VMEM((t_cols, LANES), BF16),
            pltpu.VMEM((2, 2, rows_q, q_half), BF16),
            pltpu.VMEM((width, LANES), F32),
            pltpu.VMEM((nz, 8, LANES), F32),
            pltpu.VMEM((8, 8, LANES), F32),
            pltpu.VMEM((4, 8, LANES), F32),
            pltpu.VMEM((width,), F32),
            pltpu.SMEM((4,), F32),
            dma((pieces,)), dma((pieces,)), dma((pieces,)),
            dma((33,)), dma((11,)), dma((22,)), dma((2,)),
            dma((2, nz)), dma((2, nz)), dma((8,)), dma((8,)), dma((4,)), dma((4,)), dma((3,)),
        ],
        compiler_params=pltpu.CompilerParams(
            collective_id=0, has_side_effects=True, vmem_limit_bytes=28 << 20),
    )(in_hbm(grad_rows), in_hbm(grad_query), step_count, in_hbm(down_second), in_hbm(query_second))

    return tuple(pl.pallas_call(
        finish,
        name="finish",
        out_shape=(
            jax.ShapeDtypeStruct((rows_d, width), F32),
            jax.ShapeDtypeStruct((rows_d, width), F32),
            jax.ShapeDtypeStruct((width,), F32),
            jax.ShapeDtypeStruct((rows_d, width), BF16),
            jax.ShapeDtypeStruct((rows_q, q_width), F32),
            jax.ShapeDtypeStruct((rows_q, q_width), F32),
            jax.ShapeDtypeStruct((4,), F32),
            jax.ShapeDtypeStruct((rows_q, q_width), BF16),
        ),
        in_specs=[vmem] * 8,
        out_specs=(hbm, hbm, vmem, hbm, hbm, hbm, vmem, hbm),
        scratch_shapes=[
            pltpu.VMEM((rows_d, width), F32),
            pltpu.VMEM((rows_d, width), F32),
            pltpu.VMEM((rows_d, width), BF16),
            pltpu.VMEM((rows_q, q_width), F32),
            pltpu.VMEM((rows_q, q_width), F32),
            pltpu.VMEM((rows_q, q_width), BF16),
            dma((3 * (TILES + 2),)),
        ],
        compiler_params=pltpu.CompilerParams(vmem_limit_bytes=24 << 20),
    )(n, g, t, q, down_param, down_moment, query_param, query_moment))


def solution(mesh):
    in_specs = (
        P("dp", "tensor", "ctx"),
        P("dp", "ctx", "tensor"),
        P(("tensor", "dp"), "ctx"),
        P(("tensor", "dp"), "ctx"),
        P("ctx"),
        P(("ctx", "dp"), "tensor"),
        P(("ctx", "dp"), "tensor"),
        P("tensor"),
        P(),
    )
    out_specs = (
        P(("tensor", "dp"), "ctx"),
        P(("tensor", "dp"), "ctx"),
        P("ctx"),
        P(("tensor", "dp"), "ctx"),
        P(("ctx", "dp"), "tensor"),
        P(("ctx", "dp"), "tensor"),
        P("tensor"),
        P(("ctx", "dp"), "tensor"),
    )
    body = functools.partial(shards, mesh.shape["ctx"])
    return jax.shard_map(body, mesh=mesh, in_specs=in_specs, out_specs=out_specs, check_vma=False)
```

```python
import functools
import math

import jax
import jax.numpy as jnp
from jax import lax
from jax.experimental import pallas as pl
from jax.experimental.pallas import tpu as pltpu
from jax.sharding import PartitionSpec as P

D = 4608
HEAD_DIM = 128
FF = 18432

BETA_ONE = 0.9
BETA_TWO = 0.95
EPSILON = 1e-08
LEARN_RATE = 0.003
DECAY_RATE = 0.1

MESH = pl.DeviceIdType.MESH
F32 = jnp.float32
BF16 = jnp.bfloat16

FAR, RIGHT, LEFT, SELF = range(4)
PLUS, MINUS = range(2)
LANES = 128
TILES = 4


def exchange(
    nz,
    gd, gq, dm, qm, steps, dsec, qsec,
    m_out, qm_out, n_out,
    own_d, prt_d, own_t, prt_t, own_q, prt_q,
    snd_a, snd_b, snd_t, snd_q, rly_a, rly_b, rly_t, rly_q,
    fin_pa, fin_pb, fin_ma, fin_mb, fin_tp, fin_tm, fin_q,
    tbuf, zbuf, zsend, dbuf, xbuf, m_buf, qm_buf, dsec_v, qsec_v,
    own_sem, ds_sem, dr_sem, ss, rs_rly, rs_fin, tsem, zs, zr, ps, pr, xs, xr, small_sem, hx, hz,
):
    dp, tp, cp = lax.axis_index("dp"), lax.axis_index("tensor"), lax.axis_index("ctx")
    y, core = dp // 2, dp % 2
    cols_all, wide = own_d.shape[1], own_d.shape[2]
    cut = 2 * LANES
    rest = cols_all - cut
    t_cols = cols_all // 2
    pair = 2 * wide + LANES
    rows_q, q_cols = own_q.shape[1], own_q.shape[2]
    q_half = q_cols // 2
    at = {FAR: (y + 2) % 4, RIGHT: (y + 1) % 4, LEFT: (y + 3) % 4, SELF: y}
    partner = y * 2 + (1 - core)

    def tell(sem, *device):
        pl.semaphore_signal(sem, inc=1, device_id=device, device_id_type=MESH)

    barrier = pltpu.get_barrier_semaphore()
    tell(barrier, partner, tp, cp)
    for k in (1, 3):
        tell(barrier, ((y + k) % 4) * 2 + core, tp, cp)
    for k in (1, 3):
        tell(barrier, dp, (tp + k) % 4, cp)

    @pl.when(cp > 0)
    def _():
        tell(barrier, dp, tp, cp - 1)

    @pl.when(cp < nz - 1)
    def _():
        tell(barrier, dp, tp, cp + 1)

    span = {"A": (0, cut), "B": (cut, rest), "AB": (0, cols_all)}

    def main_piece(role, who, part, first, tiles):
        row, count = span[part]
        lanes = pl.multiple_of(at[role] * pair + who * (wide + LANES) + first * LANES, LANES)
        return gd.at[0, pl.ds(row, count), pl.ds(lanes, tiles * LANES)]

    def tile_piece(role, who):
        lanes = pl.multiple_of(at[role] * pair + wide, LANES)
        return gd.at[0, pl.ds(pl.multiple_of(who * t_cols, 16), t_cols), pl.ds(lanes, LANES)]

    def query_piece(role, who):
        return gq.at[0, pl.ds(pl.multiple_of((at[role] * 2 + who) * rows_q, 8), rows_q), :]

    order = [("q", FAR), ("q", RIGHT), ("q", LEFT), ("t", FAR)] + [("d", FAR, "AB", k, 1) for k in range(TILES)]
    order += [("d", RIGHT, "B", 0, TILES), ("t", LEFT), ("d", LEFT, "A", 0, TILES)]
    order += [("t", RIGHT), ("d", RIGHT, "A", 0, TILES), ("d", LEFT, "B", 0, TILES)]
    order += [("q", SELF), ("t", SELF), ("d", SELF, "AB", 0, TILES)]

    def piece(item, who):
        if item[0] == "q":
            return query_piece(item[1], who)
        if item[0] == "t":
            return tile_piece(item[1], who)
        return main_piece(item[1], who, *item[2:])

    def landing(item, d, t, q):
        if item[0] == "q":
            return q.at[item[1]]
        if item[0] == "t":
            return t.at[item[1]]
        _, role, part, first, tiles = item
        row, count = span[part]
        return d.at[role, pl.ds(row, count), pl.ds(first * LANES, tiles * LANES)]

    own_copy = [
        pltpu.make_async_copy(piece(item, core), landing(item, own_d, own_t, own_q), own_sem.at[n])
        for n, item in enumerate(order)
    ]
    for copy in own_copy:
        copy.start()

    pl.semaphore_wait(barrier, 5 + jnp.where(cp > 0, 1, 0) + jnp.where(cp < nz - 1, 1, 0))

    prt_copy = [
        pltpu.make_async_remote_copy(
            src_ref=piece(item, 1 - core), dst_ref=landing(item, prt_d, prt_t, prt_q),
            send_sem=ds_sem.at[n], recv_sem=dr_sem.at[n],
            device_id=(partner, tp, cp), device_id_type=MESH)
        for n, item in enumerate(order)
    ]
    for copy in prt_copy:
        copy.start()

    tell(hx, dp, (tp + 3) % 4, cp)

    @pl.when(jnp.logical_and(cp > 0, cp < nz - 1))
    def _():
        tell(hz.at[0], dp, tp, cp - 1)
        tell(hz.at[1], dp, tp, cp + 1)

    small = [
        pltpu.make_async_copy(dsec, dsec_v, small_sem.at[0]),
        pltpu.make_async_copy(qsec, qsec_v, small_sem.at[1]),
        pltpu.make_async_copy(dm, m_buf, small_sem.at[2]),
        pltpu.make_async_copy(qm, qm_buf, small_sem.at[3]),
    ]
    for copy in small:
        copy.start()

    have = set()

    def need(test):
        for n, item in enumerate(order):
            if n not in have and test(item):
                have.add(n)
                own_copy[n].wait()
                prt_copy[n].wait_recv()

    def main_sum(role, part, k):
        need(lambda item: item[0] == "d" and item[1] == role and part in item[2] and item[3] <= k < item[3] + item[4])
        row, count = span[part]
        here = (role, pl.ds(row, count), pl.ds(k * LANES, LANES))
        return own_d[here].astype(F32) + prt_d[here].astype(F32)

    def tile_sum(role):
        need(lambda item: item == ("t", role))
        return own_t[role].astype(F32) + prt_t[role].astype(F32)

    def query_sum(role, block):
        need(lambda item: item == ("q", role))
        here = (role, slice(None), pl.ds(block * q_half, q_half))
        return own_q[here].astype(F32) + prt_q[here].astype(F32)

    y_copies = []
    counters = {"s": 0, "r": 0, "f": 0}

    def y_send(direction, src, dst, landing_sems, kind):
        target = at[RIGHT] if direction == PLUS else at[LEFT]
        s, r = counters["s"], counters[kind]
        counters["s"] += 1
        counters[kind] += 1
        copy = pltpu.make_async_remote_copy(
            src_ref=src, dst_ref=dst, send_sem=ss.at[s], recv_sem=landing_sems.at[r],
            device_id=(target * 2 + core, tp, cp), device_id_type=MESH)
        copy.start()
        y_copies.append(copy)
        return copy

    relayed, plain, joined = {}, {}, {}

    def store_send(direction, value, src, dst, landing_sems, kind):
        src[...] = value.astype(BF16)
        return y_send(direction, src, dst, landing_sems, kind)

    def first_q():
        for way in (PLUS, MINUS):
            relayed[way, "q"] = store_send(way, query_sum(FAR, way), snd_q.at[way, 0], rly_q.at[way], rs_rly, "r")

    def second_q():
        for way, role in ((PLUS, RIGHT), (MINUS, LEFT)):
            plain[way, "q"] = store_send(way, query_sum(role, 1 - way), snd_q.at[way, 1], fin_q.at[way, 0], rs_fin, "f")

    def third_q():
        for way, role in ((PLUS, RIGHT), (MINUS, LEFT)):
            relayed[way, "q"].wait_recv()
            value = query_sum(role, way) + rly_q[way].astype(F32)
            joined[way, "q"] = store_send(way, value, snd_q.at[way, 2], fin_q.at[way, 1], rs_fin, "f")

    def first_t():
        relayed["t"] = store_send(PLUS, tile_sum(FAR), snd_t.at[0], rly_t, rs_rly, "r")

    def second_t():
        plain["t"] = store_send(MINUS, tile_sum(LEFT), snd_t.at[1], fin_tm, rs_fin, "f")

    def third_t():
        relayed["t"].wait_recv()
        value = tile_sum(RIGHT) + rly_t[...].astype(F32)
        joined["t"] = store_send(PLUS, value, snd_t.at[2], fin_tp, rs_fin, "f")

    def first_d(k):
        relayed[PLUS, k] = store_send(PLUS, main_sum(FAR, "A", k), snd_a.at[0, k], rly_a.at[k], rs_rly, "r")
        relayed[MINUS, k] = store_send(MINUS, main_sum(FAR, "B", k), snd_b.at[0, k], rly_b.at[k], rs_rly, "r")

    def second_d(k):
        plain[PLUS, k] = store_send(PLUS, main_sum(RIGHT, "B", k), snd_b.at[1, k], fin_pb.at[k], rs_fin, "f")
        plain[MINUS, k] = store_send(MINUS, main_sum(LEFT, "A", k), snd_a.at[1, k], fin_ma.at[k], rs_fin, "f")

    def third_d(k):
        relayed[PLUS, k].wait_recv()
        value = main_sum(RIGHT, "A", k) + rly_a[k].astype(F32)
        joined[PLUS, k] = store_send(PLUS, value, snd_a.at[2, k], fin_pa.at[k], rs_fin, "f")
        relayed[MINUS, k].wait_recv()
        value = main_sum(LEFT, "B", k) + rly_b[k].astype(F32)
        joined[MINUS, k] = store_send(MINUS, value, snd_b.at[2, k], fin_mb.at[k], rs_fin, "f")

    first_q()
    second_q()
    first_t()
    first_d(0)
    third_q()
    first_d(1)
    first_d(2)
    first_d(3)
    second_t()
    for k in range(TILES):
        second_d(k)
    third_t()
    for k in range(TILES):
        third_d(k)

    for copy in small:
        copy.wait()

    def moment(old, mean):
        return BETA_ONE * old + (1.0 - BETA_ONE) * mean

    head_row = jnp.zeros((1, LANES), F32)
    lane = lax.broadcasted_iota(jnp.int32, (1, LANES), 1)
    for block in (0, 1):
        joined[block, "q"].wait_recv()
        plain[1 - block, "q"].wait_recv()
        mean = (query_sum(SELF, block) + fin_q[block, 1].astype(F32) + fin_q[1 - block, 0].astype(F32)) / 8
        here = (slice(None), pl.ds(block * q_half, q_half))
        qm_out[here] = moment(qm_buf[here], mean)
        square = jnp.sum(mean * mean, axis=0, keepdims=True)
        for h in range(2):
            part = jnp.sum(square[:, h * LANES:(h + 1) * LANES], axis=1, keepdims=True)
            head_row = jnp.where(lane == block * 2 + h, part, head_row)

    def z_copy(i):
        step = 1 << i
        peer = cp + step * (1 - 2 * ((cp // step) % 2))
        return pltpu.make_async_remote_copy(
            src_ref=zsend.at[i], dst_ref=zbuf.at[i], send_sem=zs.at[i], recv_sem=zr.at[i],
            device_id=(dp, tp, peer), device_id_type=MESH)

    @pl.when(cp <= nz - 3)
    def _():
        pl.semaphore_wait(hz.at[0], 1)

    @pl.when(cp >= 2)
    def _():
        pl.semaphore_wait(hz.at[1], 1)

    @pl.when(jnp.logical_and(cp >= 2, cp <= nz - 3))
    def _():
        tell(hz.at[2], dp, tp, cp - 2)
        tell(hz.at[2], dp, tp, cp + 2)

    z_copies = [z_copy(i) for i in range(3)]
    zsend[0] = jnp.broadcast_to(head_row, (8, LANES))
    z_copies[0].start()
    for i in (1, 2):
        z_copies[i - 1].wait_recv()
        zsend[i] = zsend[i - 1] + zbuf[i - 1]
        if i == 2:
            pl.semaphore_wait(hz.at[2], 1)
        z_copies[i].start()

    joined["t"].wait_recv()
    plain["t"].wait_recv()
    mine = pl.ds(pl.multiple_of(core * t_cols, 8), t_cols)
    tbuf[mine, :] = (tile_sum(SELF) + fin_tp[...].astype(F32) + fin_tm[...].astype(F32)) / 8
    swap = pltpu.make_async_remote_copy(
        src_ref=tbuf.at[mine, :], dst_ref=tbuf.at[mine, :], send_sem=tsem.at[0], recv_sem=tsem.at[1],
        device_id=(partner, tp, cp), device_id_type=MESH)
    swap.start()

    def column_squares(rows):
        return jnp.sum(rows * rows, axis=0, keepdims=True)

    sums_a, sums_b = jnp.zeros((1, cut), F32), jnp.zeros((1, rest), F32)
    for k in range(TILES):
        if k == 1:
            swap.wait_recv()
            both = jnp.transpose(tbuf[...])
            own_rows = jnp.where(core == 0, both[:LANES // 2], both[LANES // 2:])
            there = pl.ds(pl.multiple_of((1 - core) * wide, LANES // 2), LANES // 2)
            m_out[there, :] = moment(m_buf[there, :], own_rows)
            sums_a = sums_a + column_squares(own_rows[:, :cut])
            sums_b = sums_b + column_squares(own_rows[:, cut:])
        plain[MINUS, k].wait_recv()
        joined[PLUS, k].wait_recv()
        mean = (main_sum(SELF, "A", k) + fin_pa[k].astype(F32) + fin_ma[k].astype(F32)) / 8
        rows = jnp.transpose(mean)
        here = pl.ds(pl.multiple_of(core * (LANES // 2) + k * LANES, LANES // 2), LANES)
        m_out[here, pl.ds(0, cut)] = moment(m_buf[here, pl.ds(0, cut)], rows)
        sums_a = sums_a + column_squares(rows)
        plain[PLUS, k].wait_recv()
        joined[MINUS, k].wait_recv()
        mean = (main_sum(SELF, "B", k) + fin_mb[k].astype(F32) + fin_pb[k].astype(F32)) / 8
        rows = jnp.transpose(mean)
        m_out[here, pl.ds(cut, rest)] = moment(m_buf[here, pl.ds(cut, rest)], rows)
        sums_b = sums_b + column_squares(rows)

    z_copies[2].wait_recv()
    head_sum = zsend[2, pl.ds(0, 1), :] + zbuf[2, pl.ds(0, 1), :]

    dbuf[dp] = jnp.zeros((8, LANES), F32)
    dbuf[dp, pl.ds(0, 1), :] = sums_a[:, :LANES]
    dbuf[dp, pl.ds(1, 1), :] = sums_a[:, LANES:]
    dbuf[dp, pl.ds(2, 1), :] = sums_b[:, :LANES]
    dbuf[dp, pl.ds(3, 1), :] = sums_b[:, LANES:2 * LANES]
    dbuf[dp, pl.ds(4, 1), pl.ds(0, LANES // 2)] = sums_b[:, 2 * LANES:]
    dbuf[dp, pl.ds(5, 1), :] = head_sum

    def to_all(buf, me, size, device, send, recv):
        sends = []
        for k in range(1, size):
            copy = pltpu.make_async_remote_copy(
                src_ref=buf.at[me], dst_ref=buf.at[me], send_sem=send.at[k], recv_sem=recv.at[me],
                device_id=device((me + k) % size), device_id_type=MESH)
            copy.start()
            sends.append(copy)
        for k in range(1, size):
            other = (me + k) % size
            pltpu.make_async_remote_copy(
                src_ref=buf.at[other], dst_ref=buf.at[other], send_sem=send.at[k], recv_sem=recv.at[other],
                device_id=device(other), device_id_type=MESH).wait_recv()
        total = buf[0]
        for p in range(1, size):
            total = total + buf[p]
        return total, sends

    step = jnp.full((1, LANES), steps[0], jnp.int32).astype(F32)
    keep_one = 1.0 - jnp.exp(step * math.log(BETA_ONE))
    keep_two = 1.0 - jnp.exp(step * math.log(BETA_TWO))

    part, p_copies = to_all(dbuf, dp, 8, lambda p: (p, tp, cp), ps, pr)
    xbuf[tp] = part
    pl.semaphore_wait(hx, 1)
    whole, x_copies = to_all(xbuf, tp, 4, lambda t: (dp, t, cp), xs, xr)

    def advance(old, mean, n):
        new = BETA_TWO * old + (1.0 - BETA_TWO) * mean
        n_out[n:n + 1, :] = 1.0 / (keep_one * (jnp.sqrt(new / keep_two) + EPSILON))
        n_out[n + 8:n + 9, :] = new

    n_out[...] = jnp.zeros(n_out.shape, F32)
    for k in range(5):
        if k < 4:
            old = dsec_v[pl.ds(k * LANES, LANES)].reshape(1, LANES)
        else:
            old = dsec_v[pl.ds(k * LANES, LANES // 2)].reshape(1, LANES // 2)
            old = jnp.concatenate([old, jnp.ones((1, LANES // 2), F32)], axis=1)
        advance(old, whole[k:k + 1, :] / FF, k)
    old = jnp.ones((1, LANES), F32)
    for h in range(4):
        old = jnp.where(lane == h, qsec_v[h], old)
    advance(old, part[5:6, :] / (D * HEAD_DIM), 5)

    for copy in prt_copy + y_copies + z_copies + [swap] + p_copies + x_copies:
        copy.wait_send()


def finish(
    n_in, m_in, qm_in, dp_in, qp_in,
    dp_out, dm_out, ds_out, du_out, qp_out, qm_out, qs_out, qu_out,
    po_buf, uo_buf, qpo, quo, out_sem,
):
    rows_d, width = dp_in.shape
    stores = []

    def store(src, dst):
        copy = pltpu.make_async_copy(src, dst, out_sem.at[len(stores)])
        copy.start()
        stores.append(copy)

    def update(param, moment, scale):
        step = moment * scale
        param_new = param - LEARN_RATE * (step + DECAY_RATE * param)
        return param_new, step.astype(BF16)

    block = rows_d // 4
    store(m_in.at[pl.ds(0, 2 * block), :], dm_out.at[pl.ds(0, 2 * block), :])
    for b in range(4):
        rows = pl.ds(b * block, block)
        for k in range(5):
            lanes = pl.ds(k * LANES, LANES if k < 4 else width - 4 * LANES)
            po_buf[rows, lanes], uo_buf[rows, lanes] = update(
                dp_in[rows, lanes], m_in[rows, lanes], n_in[k:k + 1, :lanes.size])
        store(po_buf.at[rows, :], dp_out.at[rows, :])
        store(uo_buf.at[rows, :], du_out.at[rows, :])
        if b == 0:
            store(m_in.at[pl.ds(2 * block, 2 * block), :], dm_out.at[pl.ds(2 * block, 2 * block), :])
            store(qm_in, qm_out)
    for h in range(4):
        lanes = pl.ds(h * LANES, LANES)
        qpo[:, lanes], quo[:, lanes] = update(qp_in[:, lanes], qm_in[:, lanes], n_in[5:6, h:h + 1])
    store(qpo, qp_out)
    store(quo, qu_out)
    for k in range(5):
        count = LANES if k < 4 else width - 4 * LANES
        ds_out[pl.ds(k * LANES, count)] = n_in[8 + k:9 + k, :count].reshape(count)
    qs_out[...] = n_in[13:14, :4].reshape(4)
    for copy in stores:
        copy.wait()


def shards(nz, grad_down, grad_query, down_param, down_moment, down_second,
           query_param, query_moment, query_second, step_count):
    rows_d, width = down_param.shape
    rows_q, q_width = query_param.shape
    cut, wide = 2 * LANES, TILES * LANES
    rest, t_cols, q_half = width - cut, width // 2, q_width // 2
    hbm = pl.BlockSpec(memory_space=pltpu.HBM)
    vmem = pl.BlockSpec(memory_space=pltpu.VMEM)
    dma = pltpu.SemaphoreType.DMA
    pieces = 17
    grad_rows = jnp.swapaxes(grad_down, 1, 2)
    in_hbm = lambda x: pltpu.with_memory_space_constraint(x, pltpu.HBM)
    m, q_m, n = pl.pallas_call(
        functools.partial(exchange, nz),
        name="exchange",
        out_shape=(
            jax.ShapeDtypeStruct((rows_d, width), F32),
            jax.ShapeDtypeStruct((rows_q, q_width), F32),
            jax.ShapeDtypeStruct((16, LANES), F32),
        ),
        in_specs=[hbm, hbm, hbm, hbm, pl.BlockSpec(memory_space=pltpu.SMEM), hbm, hbm],
        out_specs=(vmem,) * 3,
        scratch_shapes=[
            pltpu.VMEM((4, width, wide), BF16),
            pltpu.VMEM((4, width, wide), BF16),
            pltpu.VMEM((4, t_cols, LANES), BF16),
            pltpu.VMEM((4, t_cols, LANES), BF16),
            pltpu.VMEM((4, rows_q, q_width), BF16),
            pltpu.VMEM((4, rows_q, q_width), BF16),
            pltpu.VMEM((3, TILES, cut, LANES), BF16),
            pltpu.VMEM((3, TILES, rest, LANES), BF16),
            pltpu.VMEM((3, t_cols, LANES), BF16),
            pltpu.VMEM((2, 3, rows_q, q_half), BF16),
            pltpu.VMEM((TILES, cut, LANES), BF16),
            pltpu.VMEM((TILES, rest, LANES), BF16),
            pltpu.VMEM((t_cols, LANES), BF16),
            pltpu.VMEM((2, rows_q, q_half), BF16),
            pltpu.VMEM((TILES, cut, LANES), BF16),
            pltpu.VMEM((TILES, rest, LANES), BF16),
            pltpu.VMEM((TILES, cut, LANES), BF16),
            pltpu.VMEM((TILES, rest, LANES), BF16),
            pltpu.VMEM((t_cols, LANES), BF16),
            pltpu.VMEM((t_cols, LANES), BF16),
            pltpu.VMEM((2, 2, rows_q, q_half), BF16),
            pltpu.VMEM((width, LANES), F32),
            pltpu.VMEM((3, 8, LANES), F32),
            pltpu.VMEM((3, 8, LANES), F32),
            pltpu.VMEM((8, 8, LANES), F32),
            pltpu.VMEM((4, 8, LANES), F32),
            pltpu.VMEM((rows_d, width), F32),
            pltpu.VMEM((rows_q, q_width), F32),
            pltpu.VMEM((width,), F32),
            pltpu.SMEM((4,), F32),
            dma((pieces,)), dma((pieces,)), dma((pieces,)),
            dma((33,)), dma((11,)), dma((22,)), dma((2,)),
            dma((3,)), dma((3,)), dma((8,)), dma((8,)), dma((4,)), dma((4,)), dma((4,)),
            pltpu.SemaphoreType.REGULAR, pltpu.SemaphoreType.REGULAR((3,)),
        ],
        compiler_params=pltpu.CompilerParams(
            collective_id=0, has_side_effects=True, vmem_limit_bytes=28 << 20),
    )(in_hbm(grad_rows), in_hbm(grad_query), in_hbm(down_moment), in_hbm(query_moment), step_count,
      in_hbm(down_second), in_hbm(query_second))

    return tuple(pl.pallas_call(
        finish,
        name="finish",
        out_shape=(
            jax.ShapeDtypeStruct((rows_d, width), F32),
            jax.ShapeDtypeStruct((rows_d, width), F32),
            jax.ShapeDtypeStruct((width,), F32),
            jax.ShapeDtypeStruct((rows_d, width), BF16),
            jax.ShapeDtypeStruct((rows_q, q_width), F32),
            jax.ShapeDtypeStruct((rows_q, q_width), F32),
            jax.ShapeDtypeStruct((4,), F32),
            jax.ShapeDtypeStruct((rows_q, q_width), BF16),
        ),
        in_specs=[vmem] * 5,
        out_specs=(hbm, hbm, vmem, hbm, hbm, hbm, vmem, hbm),
        scratch_shapes=[
            pltpu.VMEM((rows_d, width), F32),
            pltpu.VMEM((rows_d, width), BF16),
            pltpu.VMEM((rows_q, q_width), F32),
            pltpu.VMEM((rows_q, q_width), BF16),
            dma((13,)),
        ],
        compiler_params=pltpu.CompilerParams(vmem_limit_bytes=24 << 20),
    )(n, m, q_m, down_param, query_param))


def solution(mesh):
    in_specs = (
        P("dp", "tensor", "ctx"),
        P("dp", "ctx", "tensor"),
        P(("tensor", "dp"), "ctx"),
        P(("tensor", "dp"), "ctx"),
        P("ctx"),
        P(("ctx", "dp"), "tensor"),
        P(("ctx", "dp"), "tensor"),
        P("tensor"),
        P(),
    )
    out_specs = (
        P(("tensor", "dp"), "ctx"),
        P(("tensor", "dp"), "ctx"),
        P("ctx"),
        P(("tensor", "dp"), "ctx"),
        P(("ctx", "dp"), "tensor"),
        P(("ctx", "dp"), "tensor"),
        P("tensor"),
        P(("ctx", "dp"), "tensor"),
    )
    body = functools.partial(shards, mesh.shape["ctx"])
    return jax.shard_map(body, mesh=mesh, in_specs=in_specs, out_specs=out_specs, check_vma=False)
```

```python
import functools
import math

import jax
import jax.numpy as jnp
from jax import lax
from jax.experimental import pallas as pl
from jax.experimental.pallas import tpu as pltpu
from jax.sharding import PartitionSpec as P

D = 4608
HEAD_DIM = 128
FF = 18432

BETA_ONE = 0.9
BETA_TWO = 0.95
EPSILON = 1e-08
LEARN_RATE = 0.003
DECAY_RATE = 0.1

MESH = pl.DeviceIdType.MESH
F32 = jnp.float32
BF16 = jnp.bfloat16

FAR, RIGHT, LEFT, SELF = range(4)
PLUS, MINUS = range(2)
LANES = 128
TILES = 4


def exchange(
    nz,
    gd, gq, dm, qm, steps, dsec, qsec,
    m_out, qm_out, n_out,
    own_d, prt_d, own_t, prt_t, own_q, prt_q,
    snd_a, snd_b, snd_t, snd_q, rly_a, rly_b, rly_t, rly_q,
    fin_pa, fin_pb, fin_ma, fin_mb, fin_tp, fin_tm, fin_q,
    acc, stage_d, stage_t, stage_q, tbuf, zbuf, zsend, dbuf, m_buf, qm_buf, dsec_v, qsec_v,
    own_sem, ds_sem, dr_sem, ss, rs_rly, rs_fin, tsem, zs, zr, ps, pr, small_sem, stage_sem, hx, hz, rc, ry, rx,
):
    dp, tp, cp = lax.axis_index("dp"), lax.axis_index("tensor"), lax.axis_index("ctx")
    y, core = dp // 2, dp % 2
    cols_all, wide = own_d.shape[1], own_d.shape[2]
    cut = 2 * LANES
    rest = cols_all - cut
    t_cols = cols_all // 2
    pair = 2 * wide + LANES
    rows_q, q_cols = own_q.shape[1], own_q.shape[2]
    q_half = q_cols // 2
    at = {FAR: (y + 2) % 4, RIGHT: (y + 1) % 4, LEFT: (y + 3) % 4, SELF: y}
    partner = y * 2 + (1 - core)

    def tell(sem, *device):
        pl.semaphore_signal(sem, inc=1, device_id=device, device_id_type=MESH)

    barrier = pltpu.get_barrier_semaphore()

    @pl.when(core == 1)
    def _():
        tell(barrier, partner, tp, cp)

    @pl.when(y < 3)
    def _():
        tell(barrier, dp + 2, tp, cp)

    @pl.when(y == 0)
    def _():
        tell(barrier, 6 + core, tp, cp)

    @pl.when(tp < 3)
    def _():
        tell(barrier, dp, tp + 1, cp)

    @pl.when(tp == 0)
    def _():
        tell(barrier, dp, 3, cp)

    @pl.when(cp < nz - 1)
    def _():
        tell(barrier, dp, tp, cp + 1)

    def one_if(test):
        return jnp.where(test, 1, 0)

    greeted = (1 - core) + one_if(y > 0) + one_if(y == 3) + one_if(tp > 0) + one_if(tp == 3) + one_if(cp > 0)

    span = {"A": (0, cut), "B": (cut, rest), "AB": (0, cols_all)}

    def main_piece(role, who, part, first, tiles):
        row, count = span[part]
        lanes = pl.multiple_of(at[role] * pair + who * (wide + LANES) + first * LANES, LANES)
        return gd.at[0, pl.ds(row, count), pl.ds(lanes, tiles * LANES)]

    def tile_piece(role, who):
        lanes = pl.multiple_of(at[role] * pair + wide, LANES)
        return gd.at[0, pl.ds(pl.multiple_of(who * t_cols, 16), t_cols), pl.ds(lanes, LANES)]

    def query_piece(role, who):
        return gq.at[0, pl.ds(pl.multiple_of((at[role] * 2 + who) * rows_q, 8), rows_q), :]

    order = [("q", FAR), ("q", RIGHT), ("q", LEFT), ("t", FAR)] + [("d", FAR, "AB", k, 1) for k in range(TILES)]
    order += [("d", RIGHT, "B", 0, TILES), ("t", LEFT), ("d", LEFT, "A", 0, TILES)]
    order += [("t", RIGHT), ("d", RIGHT, "A", 0, TILES), ("d", LEFT, "B", 0, TILES)]
    order += [("q", SELF), ("t", SELF), ("d", SELF, "AB", 0, TILES)]

    def piece(item, who):
        if item[0] == "q":
            return query_piece(item[1], who)
        if item[0] == "t":
            return tile_piece(item[1], who)
        return main_piece(item[1], who, *item[2:])

    def landing(item, d, t, q):
        if item[0] == "q":
            return q.at[item[1]]
        if item[0] == "t":
            return t.at[item[1]]
        _, role, part, first, tiles = item
        row, count = span[part]
        return d.at[role, pl.ds(row, count), pl.ds(first * LANES, tiles * LANES)]

    own_copy = [
        pltpu.make_async_copy(piece(item, core), landing(item, own_d, own_t, own_q), own_sem.at[n])
        for n, item in enumerate(order)
    ]
    held = {("q", FAR): stage_q.at[0], ("q", RIGHT): stage_q.at[1], ("q", LEFT): stage_q.at[2], ("t", FAR): stage_t,
            ("d", FAR, "AB", 0, 1): stage_d}
    stage_copy = [
        pltpu.make_async_copy(piece(item, 1 - core), held[item], stage_sem.at[n])
        for n, item in enumerate(order[:len(held)])
    ]
    for own, stage in zip(own_copy, stage_copy):
        own.start()
        stage.start()

    @pl.when(greeted > 0)
    def _():
        pl.semaphore_wait(barrier, greeted)

    @pl.when(core == 0)
    def _():
        tell(rc, partner, tp, cp)

    @pl.when(y > 0)
    def _():
        tell(ry.at[0], dp - 2, tp, cp)

    @pl.when(y == 3)
    def _():
        tell(ry.at[1], core, tp, cp)

    @pl.when(tp > 0)
    def _():
        tell(rx.at[0], dp, tp - 1, cp)

    @pl.when(tp == 3)
    def _():
        tell(rx.at[1], dp, 0, cp)

    @pl.when(cp > 0)
    def _():
        tell(hz.at[3], dp, tp, cp - 1)

    @pl.when(core == 1)
    def _():
        pl.semaphore_wait(rc, 1)

    prt_copy = [
        pltpu.make_async_remote_copy(
            src_ref=held.get(item, piece(item, 1 - core)), dst_ref=landing(item, prt_d, prt_t, prt_q),
            send_sem=ds_sem.at[n], recv_sem=dr_sem.at[n],
            device_id=(partner, tp, cp), device_id_type=MESH)
        for n, item in enumerate(order)
    ]
    for n in range(len(stage_copy)):
        stage_copy[n].wait()
        prt_copy[n].start()
    for n in range(len(stage_copy), len(order)):
        own_copy[n].start()
        prt_copy[n].start()

    small = [
        pltpu.make_async_copy(dsec, dsec_v, small_sem.at[0]),
        pltpu.make_async_copy(qsec, qsec_v, small_sem.at[1]),
        pltpu.make_async_copy(dm, m_buf, small_sem.at[2]),
        pltpu.make_async_copy(qm, qm_buf, small_sem.at[3]),
    ]
    for copy in small:
        copy.start()

    have = set()

    def need(test):
        for n, item in enumerate(order):
            if n not in have and test(item):
                have.add(n)
                own_copy[n].wait()
                prt_copy[n].wait_recv()

    def main_sum(role, part, k):
        need(lambda item: item[0] == "d" and item[1] == role and part in item[2] and item[3] <= k < item[3] + item[4])
        row, count = span[part]
        here = (role, pl.ds(row, count), pl.ds(k * LANES, LANES))
        return own_d[here].astype(F32) + prt_d[here].astype(F32)

    def tile_sum(role):
        need(lambda item: item == ("t", role))
        return own_t[role].astype(F32) + prt_t[role].astype(F32)

    def query_sum(role, block):
        need(lambda item: item == ("q", role))
        here = (role, slice(None), pl.ds(block * q_half, q_half))
        return own_q[here].astype(F32) + prt_q[here].astype(F32)

    y_copies = []
    counters = {"s": 0, "r": 0, "f": 0}

    def y_send(direction, src, dst, landing_sems, kind):
        target = at[RIGHT] if direction == PLUS else at[LEFT]
        s, r = counters["s"], counters[kind]
        counters["s"] += 1
        counters[kind] += 1
        copy = pltpu.make_async_remote_copy(
            src_ref=src, dst_ref=dst, send_sem=ss.at[s], recv_sem=landing_sems.at[r],
            device_id=(target * 2 + core, tp, cp), device_id_type=MESH)
        copy.start()
        y_copies.append(copy)
        return copy

    relayed, plain, joined = {}, {}, {}

    def store_send(direction, value, src, dst, landing_sems, kind):
        src[...] = value.astype(BF16)
        return y_send(direction, src, dst, landing_sems, kind)

    def first_q():
        for way in (PLUS, MINUS):
            @pl.when(y < 3 if way == PLUS else y == 0)
            def _():
                pl.semaphore_wait(ry.at[way], 1)

            relayed[way, "q"] = store_send(way, query_sum(FAR, way), snd_q.at[way, 0], rly_q.at[way], rs_rly, "r")

    def second_q():
        for way, role in ((PLUS, RIGHT), (MINUS, LEFT)):
            plain[way, "q"] = store_send(way, query_sum(role, 1 - way), snd_q.at[way, 1], fin_q.at[way, 0], rs_fin, "f")

    def third_q():
        for way, role in ((PLUS, RIGHT), (MINUS, LEFT)):
            relayed[way, "q"].wait_recv()
            value = query_sum(role, way) + rly_q[way].astype(F32)
            joined[way, "q"] = store_send(way, value, snd_q.at[way, 2], fin_q.at[way, 1], rs_fin, "f")

    def first_t():
        relayed["t"] = store_send(PLUS, tile_sum(FAR), snd_t.at[0], rly_t, rs_rly, "r")

    def second_t():
        plain["t"] = store_send(MINUS, tile_sum(LEFT), snd_t.at[1], fin_tm, rs_fin, "f")

    def third_t():
        relayed["t"].wait_recv()
        value = tile_sum(RIGHT) + rly_t[...].astype(F32)
        joined["t"] = store_send(PLUS, value, snd_t.at[2], fin_tp, rs_fin, "f")

    def first_d(k):
        relayed[PLUS, k] = store_send(PLUS, main_sum(FAR, "A", k), snd_a.at[0, k], rly_a.at[k], rs_rly, "r")
        relayed[MINUS, k] = store_send(MINUS, main_sum(FAR, "B", k), snd_b.at[0, k], rly_b.at[k], rs_rly, "r")

    def second_d(k):
        plain[PLUS, k] = store_send(PLUS, main_sum(RIGHT, "B", k), snd_b.at[1, k], fin_pb.at[k], rs_fin, "f")
        plain[MINUS, k] = store_send(MINUS, main_sum(LEFT, "A", k), snd_a.at[1, k], fin_ma.at[k], rs_fin, "f")

    def third_d(k):
        relayed[PLUS, k].wait_recv()
        value = main_sum(RIGHT, "A", k) + rly_a[k].astype(F32)
        joined[PLUS, k] = store_send(PLUS, value, snd_a.at[2, k], fin_pa.at[k], rs_fin, "f")
        relayed[MINUS, k].wait_recv()
        value = main_sum(LEFT, "B", k) + rly_b[k].astype(F32)
        joined[MINUS, k] = store_send(MINUS, value, snd_b.at[2, k], fin_mb.at[k], rs_fin, "f")

    first_q()
    second_q()
    first_t()
    first_d(0)
    third_q()
    first_d(1)
    first_d(2)
    first_d(3)
    second_t()
    for k in range(TILES):
        second_d(k)
    third_t()

    @pl.when(cp < nz - 1)
    def _():
        pl.semaphore_wait(hz.at[3], 1)

    @pl.when(jnp.logical_and(cp > 0, cp < nz - 1))
    def _():
        tell(hz.at[0], dp, tp, cp - 1)
        tell(hz.at[1], dp, tp, cp + 1)

    for copy in small:
        copy.wait()

    def moment(old, mean):
        return BETA_ONE * old + (1.0 - BETA_ONE) * mean

    head_row = jnp.zeros((1, LANES), F32)
    lane = lax.broadcasted_iota(jnp.int32, (1, LANES), 1)
    for block in (0, 1):
        joined[block, "q"].wait_recv()
        plain[1 - block, "q"].wait_recv()
        mean = (query_sum(SELF, block) + fin_q[block, 1].astype(F32) + fin_q[1 - block, 0].astype(F32)) / 8
        here = (slice(None), pl.ds(block * q_half, q_half))
        qm_out[here] = moment(qm_buf[here], mean)
        square = jnp.sum(mean * mean, axis=0, keepdims=True)
        for h in range(2):
            part = jnp.sum(square[:, h * LANES:(h + 1) * LANES], axis=1, keepdims=True)
            head_row = jnp.where(lane == block * 2 + h, part, head_row)

    def z_copy(i):
        step = 1 << i
        peer = cp + step * (1 - 2 * ((cp // step) % 2))
        return pltpu.make_async_remote_copy(
            src_ref=zsend.at[i], dst_ref=zbuf.at[i], send_sem=zs.at[i], recv_sem=zr.at[i],
            device_id=(dp, tp, peer), device_id_type=MESH)

    z_copies = [z_copy(i) for i in range(3)]
    zsend[0] = jnp.broadcast_to(head_row, (8, LANES))
    z_copies[0].start()

    @pl.when(cp <= nz - 3)
    def _():
        pl.semaphore_wait(hz.at[0], 1)

    @pl.when(cp >= 2)
    def _():
        pl.semaphore_wait(hz.at[1], 1)

    @pl.when(jnp.logical_and(cp >= 2, cp <= nz - 3))
    def _():
        tell(hz.at[2], dp, tp, cp - 2)
        tell(hz.at[2], dp, tp, cp + 2)

    for k in range(TILES):
        third_d(k)
        if k % 2 == 1:
            i = (k + 1) // 2
            z_copies[i - 1].wait_recv()
            zsend[i] = zsend[i - 1] + zbuf[i - 1]
            if i == 2:
                pl.semaphore_wait(hz.at[2], 1)
            z_copies[i].start()

    sent = 0

    def finish_sends(upto):
        nonlocal sent
        for copy in y_copies[sent:upto]:
            copy.wait_send()
        sent = upto

    for k in range(TILES):
        plain[MINUS, k].wait_recv()
        acc[k, pl.ds(0, cut), :] = main_sum(SELF, "A", k) + fin_ma[k].astype(F32)
        plain[PLUS, k].wait_recv()
        acc[k, pl.ds(cut, rest), :] = main_sum(SELF, "B", k) + fin_pb[k].astype(F32)

    for copy in prt_copy + z_copies[:2]:
        copy.wait_send()
    finish_sends(len(y_copies) - 1 - 2 * TILES)

    joined["t"].wait_recv()
    plain["t"].wait_recv()
    mine = pl.ds(pl.multiple_of(core * t_cols, 8), t_cols)
    tbuf[mine, :] = (tile_sum(SELF) + fin_tp[...].astype(F32) + fin_tm[...].astype(F32)) / 8
    swap = pltpu.make_async_remote_copy(
        src_ref=tbuf.at[mine, :], dst_ref=tbuf.at[mine, :], send_sem=tsem.at[0], recv_sem=tsem.at[1],
        device_id=(partner, tp, cp), device_id_type=MESH)
    swap.start()

    @pl.when(tp < 3)
    def _():
        pl.semaphore_wait(rx.at[0], 1)

    @pl.when(tp == 0)
    def _():
        pl.semaphore_wait(rx.at[1], 1)

    tell(hx.at[0], dp, (tp + 3) % 4, cp)
    tell(hx.at[1], dp, (tp + 1) % 4, cp)

    def column_squares(rows):
        return jnp.sum(rows * rows, axis=0, keepdims=True)

    sums_a, sums_b = jnp.zeros((1, cut), F32), jnp.zeros((1, rest), F32)
    for k in range(TILES):
        if k == 1:
            pl.semaphore_wait(hx.at[0], 1)
            pl.semaphore_wait(hx.at[1], 1)
            tell(hx.at[2], dp, (tp + 1) % 4, cp)
            swap.wait_recv()
            both = jnp.transpose(tbuf[...])
            own_rows = jnp.where(core == 0, both[:LANES // 2], both[LANES // 2:])
            there = pl.ds(pl.multiple_of((1 - core) * wide, LANES // 2), LANES // 2)
            m_out[there, :] = moment(m_buf[there, :], own_rows)
            sums_a = sums_a + column_squares(own_rows[:, :cut])
            sums_b = sums_b + column_squares(own_rows[:, cut:])
        here = pl.ds(pl.multiple_of(core * (LANES // 2) + k * LANES, LANES // 2), LANES)
        joined[PLUS, k].wait_recv()
        rows_a = jnp.transpose((acc[k, pl.ds(0, cut), :] + fin_pa[k].astype(F32)) / 8)
        joined[MINUS, k].wait_recv()
        rows_b = jnp.transpose((acc[k, pl.ds(cut, rest), :] + fin_mb[k].astype(F32)) / 8)
        sums_a = sums_a + column_squares(rows_a)
        sums_b = sums_b + column_squares(rows_b)
        finish_sends(len(y_copies) - 2 * (TILES - k))
        if k < TILES - 1:
            m_out[here, pl.ds(0, cut)] = moment(m_buf[here, pl.ds(0, cut)], rows_a)
            m_out[here, pl.ds(cut, rest)] = moment(m_buf[here, pl.ds(cut, rest)], rows_b)
        else:
            m_out[here, pl.ds(0, cut)] = rows_a
            m_out[here, pl.ds(cut, rest)] = rows_b

    z_copies[2].wait_recv()
    head_sum = zsend[2, pl.ds(0, 1), :] + zbuf[2, pl.ds(0, 1), :]

    mine = dbuf.at[tp, dp]
    mine[pl.ds(0, 1), :] = sums_a[:, :LANES]
    mine[pl.ds(1, 1), :] = sums_a[:, LANES:]
    mine[pl.ds(2, 1), :] = sums_b[:, :LANES]
    mine[pl.ds(3, 1), :] = sums_b[:, LANES:2 * LANES]
    mine[pl.ds(4, 1), :] = jnp.concatenate([sums_b[:, 2 * LANES:], head_sum[:, :LANES // 2]], axis=1)
    pl.semaphore_wait(hx.at[2], 1)

    others = [(k, j) for k in (2, 1, 3, 0) for j in (4, 5, 2, 3, 6, 7, 1, 0) if (k, j) != (0, 0)]

    def sums_copy(n, column, row):
        return pltpu.make_async_remote_copy(
            src_ref=dbuf.at[column, row], dst_ref=dbuf.at[column, row], send_sem=ps.at[n], recv_sem=pr.at[column, row],
            device_id=((dp + others[n][1]) % 8, (tp + others[n][0]) % 4, cp), device_id_type=MESH)

    for n in range(len(others)):
        sums_copy(n, tp, dp).start()

    here = pl.ds(pl.multiple_of(core * (LANES // 2) + (TILES - 1) * LANES, LANES // 2), LANES)
    m_out[here, :] = moment(m_buf[here, :], m_out[here, :])
    step = jnp.full((1, LANES), steps[0], jnp.int32).astype(F32)
    keep_one = 1.0 - jnp.exp(step * math.log(BETA_ONE))
    keep_two = 1.0 - jnp.exp(step * math.log(BETA_TWO))
    n_out[...] = jnp.zeros(n_out.shape, F32)

    finish_sends(len(y_copies))
    swap.wait_send()
    z_copies[2].wait_send()
    for n in range(len(others)):
        sums_copy(n, tp, dp).wait_send()
    for n, (k, j) in reversed(list(enumerate(others))):
        sums_copy(n, (tp + k) % 4, (dp + j) % 8).wait_recv()

    def total(column):
        found = dbuf[column, 0]
        for p in range(1, 8):
            found = found + dbuf[column, p]
        return found

    whole = (total(0) + total(1)) + (total(2) + total(3))
    part = pltpu.roll(total(tp)[4:5, :], LANES // 2, 1)

    def advance(old, mean, n):
        new = BETA_TWO * old + (1.0 - BETA_TWO) * mean
        n_out[n:n + 1, :] = 1.0 / (keep_one * (jnp.sqrt(new / keep_two) + EPSILON))
        n_out[n + 8:n + 9, :] = new

    for k in range(5):
        if k < 4:
            old = dsec_v[pl.ds(k * LANES, LANES)].reshape(1, LANES)
        else:
            old = dsec_v[pl.ds(k * LANES, LANES // 2)].reshape(1, LANES // 2)
            old = jnp.concatenate([old, jnp.ones((1, LANES // 2), F32)], axis=1)
        advance(old, whole[k:k + 1, :] / FF, k)
    old = jnp.ones((1, LANES), F32)
    for h in range(4):
        old = jnp.where(lane == h, qsec_v[h], old)
    advance(old, part / (D * HEAD_DIM), 5)


def finish(
    n_in, m_in, qm_in, dp_in, qp_in,
    dp_out, dm_out, ds_out, du_out, qp_out, qm_out, qs_out, qu_out,
    po_buf, uo_buf, qpo, quo, out_sem,
):
    rows_d, width = dp_in.shape
    stores = []

    def store(src, dst):
        copy = pltpu.make_async_copy(src, dst, out_sem.at[len(stores)])
        copy.start()
        stores.append(copy)

    def update(param, moment, scale):
        step = moment * scale
        param_new = param - LEARN_RATE * (step + DECAY_RATE * param)
        return param_new, step.astype(BF16)

    block = rows_d // 4
    store(m_in.at[pl.ds(0, 2 * block), :], dm_out.at[pl.ds(0, 2 * block), :])
    for b in range(4):
        rows = pl.ds(b * block, block)
        for k in range(5):
            lanes = pl.ds(k * LANES, LANES if k < 4 else width - 4 * LANES)
            po_buf[rows, lanes], uo_buf[rows, lanes] = update(
                dp_in[rows, lanes], m_in[rows, lanes], n_in[k:k + 1, :lanes.size])
        store(po_buf.at[rows, :], dp_out.at[rows, :])
        store(uo_buf.at[rows, :], du_out.at[rows, :])
        if b == 0:
            store(m_in.at[pl.ds(2 * block, 2 * block), :], dm_out.at[pl.ds(2 * block, 2 * block), :])
            store(qm_in, qm_out)
    for h in range(4):
        lanes = pl.ds(h * LANES, LANES)
        qpo[:, lanes], quo[:, lanes] = update(qp_in[:, lanes], qm_in[:, lanes], n_in[5:6, h:h + 1])
    store(qpo, qp_out)
    store(quo, qu_out)
    for k in range(5):
        count = LANES if k < 4 else width - 4 * LANES
        ds_out[pl.ds(k * LANES, count)] = n_in[8 + k:9 + k, :count].reshape(count)
    qs_out[...] = n_in[13:14, :4].reshape(4)
    for copy in stores:
        copy.wait()


def shards(nz, grad_down, grad_query, down_param, down_moment, down_second,
           query_param, query_moment, query_second, step_count):
    rows_d, width = down_param.shape
    rows_q, q_width = query_param.shape
    cut, wide = 2 * LANES, TILES * LANES
    rest, t_cols, q_half = width - cut, width // 2, q_width // 2
    hbm = pl.BlockSpec(memory_space=pltpu.HBM)
    vmem = pl.BlockSpec(memory_space=pltpu.VMEM)
    dma = pltpu.SemaphoreType.DMA
    pieces = 17
    grad_rows = jnp.swapaxes(grad_down, 1, 2)
    in_hbm = lambda x: pltpu.with_memory_space_constraint(x, pltpu.HBM)
    m, q_m, n = pl.pallas_call(
        functools.partial(exchange, nz),
        name="exchange",
        out_shape=(
            jax.ShapeDtypeStruct((rows_d, width), F32),
            jax.ShapeDtypeStruct((rows_q, q_width), F32),
            jax.ShapeDtypeStruct((16, LANES), F32),
        ),
        in_specs=[hbm, hbm, hbm, hbm, pl.BlockSpec(memory_space=pltpu.SMEM), hbm, hbm],
        out_specs=(vmem,) * 3,
        scratch_shapes=[
            pltpu.VMEM((4, width, wide), BF16),
            pltpu.VMEM((4, width, wide), BF16),
            pltpu.VMEM((4, t_cols, LANES), BF16),
            pltpu.VMEM((4, t_cols, LANES), BF16),
            pltpu.VMEM((4, rows_q, q_width), BF16),
            pltpu.VMEM((4, rows_q, q_width), BF16),
            pltpu.VMEM((3, TILES, cut, LANES), BF16),
            pltpu.VMEM((3, TILES, rest, LANES), BF16),
            pltpu.VMEM((3, t_cols, LANES), BF16),
            pltpu.VMEM((2, 3, rows_q, q_half), BF16),
            pltpu.VMEM((TILES, cut, LANES), BF16),
            pltpu.VMEM((TILES, rest, LANES), BF16),
            pltpu.VMEM((t_cols, LANES), BF16),
            pltpu.VMEM((2, rows_q, q_half), BF16),
            pltpu.VMEM((TILES, cut, LANES), BF16),
            pltpu.VMEM((TILES, rest, LANES), BF16),
            pltpu.VMEM((TILES, cut, LANES), BF16),
            pltpu.VMEM((TILES, rest, LANES), BF16),
            pltpu.VMEM((t_cols, LANES), BF16),
            pltpu.VMEM((t_cols, LANES), BF16),
            pltpu.VMEM((2, 2, rows_q, q_half), BF16),
            pltpu.VMEM((TILES, width, LANES), F32),
            pltpu.VMEM((width, LANES), BF16),
            pltpu.VMEM((t_cols, LANES), BF16),
            pltpu.VMEM((3, rows_q, q_width), BF16),
            pltpu.VMEM((width, LANES), F32),
            pltpu.VMEM((3, 8, LANES), F32),
            pltpu.VMEM((3, 8, LANES), F32),
            pltpu.VMEM((4, 8, 5, LANES), F32),
            pltpu.VMEM((rows_d, width), F32),
            pltpu.VMEM((rows_q, q_width), F32),
            pltpu.VMEM((width,), F32),
            pltpu.SMEM((4,), F32),
            dma((pieces,)), dma((pieces,)), dma((pieces,)),
            dma((33,)), dma((11,)), dma((22,)), dma((2,)),
            dma((3,)), dma((3,)), dma((31,)), dma((4, 8)), dma((4,)), dma((5,)),
            pltpu.SemaphoreType.REGULAR((3,)), pltpu.SemaphoreType.REGULAR((4,)),
            pltpu.SemaphoreType.REGULAR, pltpu.SemaphoreType.REGULAR((2,)), pltpu.SemaphoreType.REGULAR((2,)),
        ],
        compiler_params=pltpu.CompilerParams(
            collective_id=0, has_side_effects=True, vmem_limit_bytes=28 << 20),
    )(in_hbm(grad_rows), in_hbm(grad_query), in_hbm(down_moment), in_hbm(query_moment), step_count,
      in_hbm(down_second), in_hbm(query_second))

    return tuple(pl.pallas_call(
        finish,
        name="finish",
        out_shape=(
            jax.ShapeDtypeStruct((rows_d, width), F32),
            jax.ShapeDtypeStruct((rows_d, width), F32),
            jax.ShapeDtypeStruct((width,), F32),
            jax.ShapeDtypeStruct((rows_d, width), BF16),
            jax.ShapeDtypeStruct((rows_q, q_width), F32),
            jax.ShapeDtypeStruct((rows_q, q_width), F32),
            jax.ShapeDtypeStruct((4,), F32),
            jax.ShapeDtypeStruct((rows_q, q_width), BF16),
        ),
        in_specs=[vmem] * 5,
        out_specs=(hbm, hbm, vmem, hbm, hbm, hbm, vmem, hbm),
        scratch_shapes=[
            pltpu.VMEM((rows_d, width), F32),
            pltpu.VMEM((rows_d, width), BF16),
            pltpu.VMEM((rows_q, q_width), F32),
            pltpu.VMEM((rows_q, q_width), BF16),
            dma((13,)),
        ],
        compiler_params=pltpu.CompilerParams(vmem_limit_bytes=24 << 20),
    )(n, m, q_m, down_param, query_param))


def solution(mesh):
    in_specs = (
        P("dp", "tensor", "ctx"),
        P("dp", "ctx", "tensor"),
        P(("tensor", "dp"), "ctx"),
        P(("tensor", "dp"), "ctx"),
        P("ctx"),
        P(("ctx", "dp"), "tensor"),
        P(("ctx", "dp"), "tensor"),
        P("tensor"),
        P(),
    )
    out_specs = (
        P(("tensor", "dp"), "ctx"),
        P(("tensor", "dp"), "ctx"),
        P("ctx"),
        P(("tensor", "dp"), "ctx"),
        P(("ctx", "dp"), "tensor"),
        P(("ctx", "dp"), "tensor"),
        P("tensor"),
        P(("ctx", "dp"), "tensor"),
    )
    body = functools.partial(shards, mesh.shape["ctx"])
    return jax.shard_map(body, mesh=mesh, in_specs=in_specs, out_specs=out_specs, check_vma=False)
```

```python
import functools
import math

import jax
import jax.numpy as jnp
from jax import lax
from jax.experimental import pallas as pl
from jax.experimental.pallas import tpu as pltpu
from jax.sharding import PartitionSpec as P

D = 4608
HEAD_DIM = 128
FF = 18432

BETA_ONE = 0.9
BETA_TWO = 0.95
EPSILON = 1e-08
LEARN_RATE = 0.003
DECAY_RATE = 0.1

MESH = pl.DeviceIdType.MESH
F32 = jnp.float32
BF16 = jnp.bfloat16

FAR, RIGHT, LEFT, SELF = range(4)
PLUS, MINUS = range(2)
LANES = 128
TILES = 4


def exchange(
    nz,
    gd, gq, dm, qm, steps, dsec, qsec,
    m_out, qm_out, n_out,
    own_d, prt_d, own_t, prt_t, own_q, prt_q,
    snd_a, snd_b, snd_t, snd_q, rly_a, rly_b, rly_t, rly_q,
    fin_pa, fin_pb, fin_ma, fin_mb, fin_t, fin_q,
    acc, stage_d, stage_t, stage_q, tbuf, zbuf, zsend, dbuf, m_buf, qm_buf, dsec_v, qsec_v,
    own_sem, ds_sem, dr_sem, ss, rly_sem, fin_sem, join_sem, tsem, zs, zr, sums_sem, small_sem, stage_sem,
    hx, hz, rc, ry, rx,
):
    div, rem = lax.div, lax.rem
    dp, tp, cp = lax.axis_index("dp"), lax.axis_index("tensor"), lax.axis_index("ctx")
    y, core = div(dp, 2), rem(dp, 2)
    cols_all, wide = own_d.shape[1], own_d.shape[2]
    cut = 2 * LANES
    rest = cols_all - cut
    t_cols = cols_all // 2
    pair = 2 * wide + LANES
    rows_q, q_cols = own_q.shape[1], own_q.shape[2]
    q_half = q_cols // 2
    at = {FAR: rem(y + 2, 4), RIGHT: rem(y + 1, 4), LEFT: rem(y + 3, 4), SELF: y}
    partner = y * 2 + (1 - core)
    after, before = rem(tp + 1, 4), rem(tp + 3, 4)

    def tell(sem, *device):
        pl.semaphore_signal(sem, inc=1, device_id=device, device_id_type=MESH)

    barrier = pltpu.get_barrier_semaphore()

    @pl.when(core == 1)
    def _():
        tell(barrier, partner, tp, cp)

    @pl.when(y < 3)
    def _():
        tell(barrier, dp + 2, tp, cp)

    @pl.when(y == 0)
    def _():
        tell(barrier, 6 + core, tp, cp)

    @pl.when(tp < 3)
    def _():
        tell(barrier, dp, tp + 1, cp)

    @pl.when(tp == 0)
    def _():
        tell(barrier, dp, 3, cp)

    @pl.when(cp < nz - 1)
    def _():
        tell(barrier, dp, tp, cp + 1)

    def one_if(test):
        return jnp.where(test, 1, 0)

    greeted = (1 - core) + one_if(y > 0) + one_if(y == 3) + one_if(tp > 0) + one_if(tp == 3) + one_if(cp > 0)

    span = {"A": (0, cut), "B": (cut, rest), "AB": (0, cols_all)}

    def main_piece(role, who, part, first, tiles):
        row, count = span[part]
        lanes = pl.multiple_of(at[role] * pair + who * (wide + LANES) + first * LANES, LANES)
        return gd.at[0, pl.ds(row, count), pl.ds(lanes, tiles * LANES)]

    def tile_piece(role, who):
        lanes = pl.multiple_of(at[role] * pair + wide, LANES)
        return gd.at[0, pl.ds(pl.multiple_of(who * t_cols, 16), t_cols), pl.ds(lanes, LANES)]

    def query_piece(role, who):
        return gq.at[0, pl.ds(pl.multiple_of((at[role] * 2 + who) * rows_q, 8), rows_q), :]

    order = [(("q", FAR), 0), (("q", RIGHT), 1), (("q", LEFT), 1), (("t", FAR), 2), (("d", FAR, "AB", 0, 1), 3)]
    order += [(("d", FAR, "AB", k, 1), 3 + k) for k in range(1, TILES)]
    order += [(("q", SELF), 11), (("t", LEFT), 7), (("t", RIGHT), 7), (("t", SELF), 7)]
    order += [(("d", RIGHT, "B", 0, TILES), 8), (("d", LEFT, "A", 0, TILES), 8)]
    order += [(("d", RIGHT, "A", 0, TILES), 9), (("d", LEFT, "B", 0, TILES), 9), (("d", SELF, "AB", 0, TILES), 10)]
    own_order = [(("q", FAR), 0), (("t", FAR), 1), (("d", FAR, "AB", 0, TILES), 2)]
    own_rest = [((kind, role), n) for n, kind in ((3, "q"), (4, "t")) for role in (RIGHT, LEFT, SELF)]
    own_rest += [(("d", role, "AB", 0, TILES), 5) for role in (RIGHT, LEFT, SELF)]

    def piece(item, who):
        if item[0] == "q":
            return query_piece(item[1], who)
        if item[0] == "t":
            return tile_piece(item[1], who)
        return main_piece(item[1], who, *item[2:])

    def landing(item, d, t, q):
        if item[0] == "q":
            return q.at[item[1]]
        if item[0] == "t":
            return t.at[item[1]]
        _, role, part, first, tiles = item
        row, count = span[part]
        return d.at[role, pl.ds(row, count), pl.ds(first * LANES, tiles * LANES)]

    def own_load(item, n):
        pltpu.make_async_copy(piece(item, core), landing(item, own_d, own_t, own_q), own_sem.at[n]).start()

    held = {("q", FAR): (stage_q.at[0], 0), ("q", RIGHT): (stage_q.at[1], 1), ("q", LEFT): (stage_q.at[2], 1),
            ("t", FAR): (stage_t, 2), ("d", FAR, "AB", 0, 1): (stage_d, 3)}

    def stage_load(item):
        pltpu.make_async_copy(piece(item, 1 - core), held[item][0], stage_sem.at[held[item][1]]).start()

    stage_load(("q", FAR))
    own_load(*own_order[0])
    stage_load(("q", RIGHT))
    stage_load(("q", LEFT))
    stage_load(("t", FAR))
    own_load(*own_order[1])
    stage_load(("d", FAR, "AB", 0, 1))
    own_load(*own_order[2])
    for entry in own_rest[:3]:
        own_load(*entry)

    @pl.when(greeted > 0)
    def _():
        pl.semaphore_wait(barrier, greeted)

    @pl.when(core == 0)
    def _():
        tell(rc, partner, tp, cp)

    @pl.when(y > 0)
    def _():
        tell(ry.at[0], dp - 2, tp, cp)

    @pl.when(y == 3)
    def _():
        tell(ry.at[1], core, tp, cp)

    @pl.when(tp > 0)
    def _():
        tell(rx.at[0], dp, tp - 1, cp)

    @pl.when(tp == 3)
    def _():
        tell(rx.at[1], dp, 0, cp)

    @pl.when(cp > 0)
    def _():
        tell(hz.at[3], dp, tp, cp - 1)

    @pl.when(core == 1)
    def _():
        pl.semaphore_wait(rc, 1)

    kinds = {"q": 0, "t": 1, "d": 2}
    def settled(ref, sem):
        return pltpu.make_async_remote_copy(
            src_ref=ref, dst_ref=ref, send_sem=sem, recv_sem=sem, device_id=(partner, tp, cp), device_id_type=MESH)

    def prt_start(item, n):
        pltpu.make_async_remote_copy(
            src_ref=held[item][0] if item in held else piece(item, 1 - core), dst_ref=landing(item, prt_d, prt_t, prt_q),
            send_sem=ds_sem.at[kinds[item[0]]], recv_sem=dr_sem.at[n],
            device_id=(partner, tp, cp), device_id_type=MESH).start()

    for n, item in enumerate(list(held)):
        if n != 2:
            ref = stage_q.at[pl.ds(1, 2)] if n == 1 else held[item][0]
            pltpu.make_async_copy(ref, ref, stage_sem.at[held[item][1]]).wait()
        prt_start(*order[n])
    for entry in own_rest[3:6]:
        own_load(*entry)
    for entry in order[len(held):8]:
        prt_start(*entry)
    for entry in own_rest[6:]:
        own_load(*entry)
    for entry in order[8:]:
        prt_start(*entry)

    small = [
        pltpu.make_async_copy(dsec, dsec_v, small_sem.at[0]),
        pltpu.make_async_copy(qsec, qsec_v, small_sem.at[1]),
        pltpu.make_async_copy(dm, m_buf, small_sem.at[2]),
        pltpu.make_async_copy(qm, qm_buf, small_sem.at[3]),
    ]
    for copy in small:
        copy.start()

    have = set()
    three = pl.ds(RIGHT, 3)
    own_ref = [own_q.at[FAR], own_t.at[FAR], own_d.at[FAR], own_q.at[three], own_t.at[three], own_d.at[three]]
    one_tile = prt_d.at[FAR, :, pl.ds(0, LANES)]
    prt_ref = [prt_q.at[FAR], prt_q.at[pl.ds(RIGHT, 2)], prt_t.at[FAR]] + [one_tile] * 4 + [
        prt_t.at[three], prt_d.at[RIGHT], prt_d.at[RIGHT], prt_d.at[SELF], prt_q.at[SELF]]

    def need(own, prt):
        if ("own", own) not in have:
            have.add(("own", own))
            pltpu.make_async_copy(own_ref[own], own_ref[own], own_sem.at[own]).wait()
        if ("prt", prt) not in have:
            have.add(("prt", prt))
            settled(prt_ref[prt], dr_sem.at[prt]).wait_recv()

    def main_sum(role, part, k):
        if role == FAR:
            need(2, 3 + k)
        elif role == SELF:
            need(5, 10)
        else:
            need(5, 8 if (role == RIGHT) == (part == "B") else 9)
        row, count = span[part]
        where = (role, pl.ds(row, count), pl.ds(k * LANES, LANES))
        return own_d[where].astype(F32) + prt_d[where].astype(F32)

    def tile_sum(role):
        need(1, 2) if role == FAR else need(4, 7)
        return own_t[role].astype(F32) + prt_t[role].astype(F32)

    def query_sum(role, block):
        need(0, 0) if role == FAR else need(3, 11 if role == SELF else 1)
        where = (role, slice(None), pl.ds(block * q_half, q_half))
        return own_q[where].astype(F32) + prt_q[where].astype(F32)

    def y_send(way, value, src, send, dst, recv):
        src[...] = value.astype(BF16)
        pltpu.make_async_remote_copy(
            src_ref=src, dst_ref=dst, send_sem=ss.at[send], recv_sem=recv,
            device_id=((at[RIGHT] if way == PLUS else at[LEFT]) * 2 + core, tp, cp), device_id_type=MESH).start()

    def first_q():
        for way in (PLUS, MINUS):
            @pl.when(y < 3 if way == PLUS else y == 0)
            def _():
                pl.semaphore_wait(ry.at[way], 1)

            y_send(way, query_sum(FAR, way), snd_q.at[way, 0], 3, rly_q.at[way], rly_sem.at[9])

    def second_q():
        for way, role in ((PLUS, RIGHT), (MINUS, LEFT)):
            y_send(way, query_sum(role, 1 - way), snd_q.at[way, 1], 3, fin_q.at[way, 0], fin_sem.at[3])

    def third_q():
        settled(rly_q, rly_sem.at[9]).wait_recv()
        for way, role in ((PLUS, RIGHT), (MINUS, LEFT)):
            y_send(way, query_sum(role, way) + rly_q[way].astype(F32), snd_q.at[way, 2], 3, fin_q.at[way, 1], fin_sem.at[3])

    def first_t():
        y_send(PLUS, tile_sum(FAR), snd_t.at[0], 2, rly_t, rly_sem.at[8])

    def second_t():
        y_send(MINUS, tile_sum(LEFT), snd_t.at[1], 2, fin_t.at[0], fin_sem.at[2])

    def third_t():
        settled(rly_t, rly_sem.at[8]).wait_recv()
        y_send(PLUS, tile_sum(RIGHT) + rly_t[...].astype(F32), snd_t.at[2], 2, fin_t.at[1], fin_sem.at[2])

    def first_d(k):
        y_send(PLUS, main_sum(FAR, "A", k), snd_a.at[0, k], 0, rly_a.at[k], rly_sem.at[k])
        y_send(MINUS, main_sum(FAR, "B", k), snd_b.at[0, k], 1, rly_b.at[k], rly_sem.at[4 + k])

    def second_d(k):
        y_send(PLUS, main_sum(RIGHT, "B", k), snd_b.at[1, k], 1, fin_pb.at[k], fin_sem.at[0])
        y_send(MINUS, main_sum(LEFT, "A", k), snd_a.at[1, k], 0, fin_ma.at[k], fin_sem.at[1])

    def third_d(k):
        settled(rly_a.at[k], rly_sem.at[k]).wait_recv()
        y_send(PLUS, main_sum(RIGHT, "A", k) + rly_a[k].astype(F32), snd_a.at[2, k], 0, fin_pa.at[k], join_sem.at[PLUS, k])
        settled(rly_b.at[k], rly_sem.at[4 + k]).wait_recv()
        y_send(MINUS, main_sum(LEFT, "B", k) + rly_b[k].astype(F32), snd_b.at[2, k], 1, fin_mb.at[k], join_sem.at[MINUS, k])

    first_q()
    second_q()
    first_t()
    first_d(0)
    third_q()
    first_d(1)
    first_d(2)
    first_d(3)
    second_t()
    for k in range(TILES):
        second_d(k)
    third_t()

    @pl.when(cp < nz - 1)
    def _():
        pl.semaphore_wait(hz.at[3], 1)

    @pl.when(jnp.logical_and(cp > 0, cp < nz - 1))
    def _():
        tell(hz.at[0], dp, tp, cp - 1)
        tell(hz.at[1], dp, tp, cp + 1)

    for copy in small:
        copy.wait()

    def moment(old, mean):
        return BETA_ONE * old + (1.0 - BETA_ONE) * mean

    head_row = jnp.zeros((1, LANES), F32)
    lane = lax.broadcasted_iota(jnp.int32, (1, LANES), 1)
    settled(fin_q, fin_sem.at[3]).wait_recv()
    for block in (0, 1):
        mean = (query_sum(SELF, block) + fin_q[block, 1].astype(F32) + fin_q[1 - block, 0].astype(F32)) / 8
        where = (slice(None), pl.ds(block * q_half, q_half))
        qm_out[where] = moment(qm_buf[where], mean)
        square = jnp.sum(mean * mean, axis=0, keepdims=True)
        for h in range(2):
            part = jnp.sum(square[:, h * LANES:(h + 1) * LANES], axis=1, keepdims=True)
            head_row = jnp.where(lane == block * 2 + h, part, head_row)

    def z_copy(i):
        step = 1 << i
        peer = cp + step * (1 - 2 * rem(div(cp, step), 2))
        return pltpu.make_async_remote_copy(
            src_ref=zsend.at[i], dst_ref=zbuf.at[i], send_sem=zs, recv_sem=zr.at[i],
            device_id=(dp, tp, peer), device_id_type=MESH)

    z_copies = [z_copy(i) for i in range(3)]
    zsend[0] = jnp.broadcast_to(head_row, (8, LANES))
    z_copies[0].start()

    @pl.when(cp <= nz - 3)
    def _():
        pl.semaphore_wait(hz.at[0], 1)

    @pl.when(cp >= 2)
    def _():
        pl.semaphore_wait(hz.at[1], 1)

    @pl.when(jnp.logical_and(cp >= 2, cp <= nz - 3))
    def _():
        tell(hz.at[2], dp, tp, cp - 2)
        tell(hz.at[2], dp, tp, cp + 2)

    for k in range(TILES):
        third_d(k)
        if k % 2 == 1:
            i = (k + 1) // 2
            z_copies[i - 1].wait_recv()
            zsend[i] = zsend[i - 1] + zbuf[i - 1]
            if i == 2:
                pl.semaphore_wait(hz.at[2], 1)
            z_copies[i].start()

    settled(fin_ma, fin_sem.at[1]).wait_recv()
    settled(fin_pb, fin_sem.at[0]).wait_recv()
    for k in range(TILES):
        acc[k, pl.ds(0, cut), :] = main_sum(SELF, "A", k) + fin_ma[k].astype(F32)
        acc[k, pl.ds(cut, rest), :] = main_sum(SELF, "B", k) + fin_pb[k].astype(F32)
    for n, ref in enumerate((prt_q, prt_t, prt_d)):
        settled(ref, ds_sem.at[n]).wait_send()

    settled(fin_t, fin_sem.at[2]).wait_recv()
    mine = pl.ds(pl.multiple_of(core * t_cols, 8), t_cols)
    tbuf[mine, :] = (tile_sum(SELF) + fin_t[0].astype(F32) + fin_t[1].astype(F32)) / 8
    swap = pltpu.make_async_remote_copy(
        src_ref=tbuf.at[mine, :], dst_ref=tbuf.at[mine, :], send_sem=tsem.at[0], recv_sem=tsem.at[1],
        device_id=(partner, tp, cp), device_id_type=MESH)
    swap.start()

    @pl.when(tp < 3)
    def _():
        pl.semaphore_wait(rx.at[0], 1)

    @pl.when(tp == 0)
    def _():
        pl.semaphore_wait(rx.at[1], 1)

    tell(hx.at[0], dp, before, cp)
    tell(hx.at[1], dp, after, cp)
    settled(snd_q, ss.at[3]).wait_send()
    settled(snd_t, ss.at[2]).wait_send()

    def column_squares(rows):
        return jnp.sum(rows * rows, axis=0, keepdims=True)

    sums_a, sums_b = jnp.zeros((1, cut), F32), jnp.zeros((1, rest), F32)
    for k in range(TILES):
        if k == 1:
            pl.semaphore_wait(hx.at[0], 1)
            pl.semaphore_wait(hx.at[1], 1)
            tell(hx.at[2], dp, after, cp)
            swap.wait_recv()
            both = jnp.transpose(tbuf[...])
            own_rows = jnp.where(core == 0, both[:LANES // 2], both[LANES // 2:])
            there = pl.ds(pl.multiple_of((1 - core) * wide, LANES // 2), LANES // 2)
            m_out[there, :] = moment(m_buf[there, :], own_rows)
            sums_a = sums_a + column_squares(own_rows[:, :cut])
            sums_b = sums_b + column_squares(own_rows[:, cut:])
        here = pl.ds(pl.multiple_of(core * (LANES // 2) + k * LANES, LANES // 2), LANES)
        settled(fin_pa.at[k], join_sem.at[PLUS, k]).wait_recv()
        rows_a = jnp.transpose((acc[k, pl.ds(0, cut), :] + fin_pa[k].astype(F32)) / 8)
        settled(fin_mb.at[k], join_sem.at[MINUS, k]).wait_recv()
        rows_b = jnp.transpose((acc[k, pl.ds(cut, rest), :] + fin_mb[k].astype(F32)) / 8)
        sums_a = sums_a + column_squares(rows_a)
        sums_b = sums_b + column_squares(rows_b)
        if k < TILES - 1:
            m_out[here, pl.ds(0, cut)] = moment(m_buf[here, pl.ds(0, cut)], rows_a)
            m_out[here, pl.ds(cut, rest)] = moment(m_buf[here, pl.ds(cut, rest)], rows_b)
        else:
            m_out[here, pl.ds(0, cut)] = rows_a
            m_out[here, pl.ds(cut, rest)] = rows_b

    z_copies[2].wait_recv()
    head_sum = zsend[2, pl.ds(0, 1), :] + zbuf[2, pl.ds(0, 1), :]

    slot = tp * 8 + dp
    mine = dbuf.at[slot]
    mine[pl.ds(0, 1), :] = sums_a[:, :LANES]
    mine[pl.ds(1, 1), :] = sums_a[:, LANES:]
    mine[pl.ds(2, 1), :] = sums_b[:, :LANES]
    mine[pl.ds(3, 1), :] = sums_b[:, LANES:2 * LANES]
    mine[pl.ds(4, 1), :] = jnp.concatenate([sums_b[:, 2 * LANES:], head_sum[:, :LANES // 2]], axis=1)
    pl.semaphore_wait(hx.at[2], 1)

    others = [(k, j) for k in (2, 1, 3, 0) for j in (4, 5, 2, 3, 6, 7, 1, 0) if (k, j) != (0, 0)]
    for k, j in others:
        pltpu.make_async_remote_copy(
            src_ref=mine, dst_ref=mine, send_sem=sums_sem.at[0], recv_sem=sums_sem.at[1],
            device_id=(rem(dp + j, 8), rem(tp + k, 4), cp), device_id_type=MESH).start()

    here = pl.ds(pl.multiple_of(core * (LANES // 2) + (TILES - 1) * LANES, LANES // 2), LANES)
    m_out[here, :] = moment(m_buf[here, :], m_out[here, :])
    step = jnp.full((1, LANES), steps[0], jnp.int32).astype(F32)
    keep_one = 1.0 - jnp.exp(step * math.log(BETA_ONE))
    keep_two = 1.0 - jnp.exp(step * math.log(BETA_TWO))
    n_out[...] = jnp.zeros(n_out.shape, F32)

    settled(snd_a, ss.at[0]).wait_send()
    settled(snd_b, ss.at[1]).wait_send()
    swap.wait_send()
    settled(zsend, zs).wait_send()
    everyone_else = dbuf.at[pl.ds(0, len(others))]
    settled(everyone_else, sums_sem.at[0]).wait_send()
    settled(everyone_else, sums_sem.at[1]).wait_recv()

    def total(column):
        found = dbuf[column * 8]
        for p in range(1, 8):
            found = found + dbuf[column * 8 + p]
        return found

    whole = (total(0) + total(1)) + (total(2) + total(3))
    part = pltpu.roll(total(tp)[4:5, :], LANES // 2, 1)

    def advance(old, mean, n):
        new = BETA_TWO * old + (1.0 - BETA_TWO) * mean
        n_out[n:n + 1, :] = 1.0 / (keep_one * (jnp.sqrt(new / keep_two) + EPSILON))
        n_out[n + 8:n + 9, :] = new

    for k in range(5):
        if k < 4:
            old = dsec_v[pl.ds(k * LANES, LANES)].reshape(1, LANES)
        else:
            old = dsec_v[pl.ds(k * LANES, LANES // 2)].reshape(1, LANES // 2)
            old = jnp.concatenate([old, jnp.ones((1, LANES // 2), F32)], axis=1)
        advance(old, whole[k:k + 1, :] / FF, k)
    old = jnp.ones((1, LANES), F32)
    for h in range(4):
        old = jnp.where(lane == h, qsec_v[h], old)
    advance(old, part / (D * HEAD_DIM), 5)


def finish(
    n_in, m_in, qm_in, dp_in, qp_in,
    dp_out, dm_out, ds_out, du_out, qp_out, qm_out, qs_out, qu_out,
    po_buf, uo_buf, qpo, quo, ds_buf, qs_buf, out_sem,
):
    rows_d, width = dp_in.shape

    def store(n, src, dst):
        pltpu.make_async_copy(src, dst, out_sem.at[n]).start()

    def update(param, moment, scale):
        step = moment * scale
        param_new = param - LEARN_RATE * (step + DECAY_RATE * param)
        return param_new, step.astype(BF16)

    block = rows_d // 4
    store(0, m_in, dm_out)
    for k in range(5):
        count = LANES if k < 4 else width - 4 * LANES
        ds_buf[pl.ds(k * LANES, count)] = n_in[8 + k:9 + k, :count].reshape(count)
    qs_buf[...] = n_in[13:14, :4].reshape(4)
    store(1, ds_buf, ds_out)
    store(2, qs_buf, qs_out)
    for b in range(4):
        rows = pl.ds(b * block, block)
        for k in range(5):
            lanes = pl.ds(k * LANES, LANES if k < 4 else width - 4 * LANES)
            po_buf[rows, lanes], uo_buf[rows, lanes] = update(
                dp_in[rows, lanes], m_in[rows, lanes], n_in[k:k + 1, :lanes.size])
        store(3, po_buf.at[rows, :], dp_out.at[rows, :])
        store(4, uo_buf.at[rows, :], du_out.at[rows, :])
        if b == 0:
            store(5, qm_in, qm_out)
    for h in range(4):
        lanes = pl.ds(h * LANES, LANES)
        qpo[:, lanes], quo[:, lanes] = update(qp_in[:, lanes], qm_in[:, lanes], n_in[5:6, h:h + 1])
    store(6, qpo, qp_out)
    store(7, quo, qu_out)
    for n, (src, dst) in enumerate((
            (m_in, dm_out), (ds_buf, ds_out), (qs_buf, qs_out), (po_buf, dp_out), (uo_buf, du_out),
            (qm_in, qm_out), (qpo, qp_out), (quo, qu_out))):
        pltpu.make_async_copy(src, dst, out_sem.at[n]).wait()


def shards(nz, grad_down, grad_query, down_param, down_moment, down_second,
           query_param, query_moment, query_second, step_count):
    rows_d, width = down_param.shape
    rows_q, q_width = query_param.shape
    cut, wide = 2 * LANES, TILES * LANES
    rest, t_cols, q_half = width - cut, width // 2, q_width // 2
    hbm = pl.BlockSpec(memory_space=pltpu.HBM)
    vmem = pl.BlockSpec(memory_space=pltpu.VMEM)
    dma = pltpu.SemaphoreType.DMA
    regular = pltpu.SemaphoreType.REGULAR
    grad_rows = jnp.swapaxes(grad_down, 1, 2)
    in_hbm = lambda x: pltpu.with_memory_space_constraint(x, pltpu.HBM)
    m, q_m, n = pl.pallas_call(
        functools.partial(exchange, nz),
        name="exchange",
        out_shape=(
            jax.ShapeDtypeStruct((rows_d, width), F32),
            jax.ShapeDtypeStruct((rows_q, q_width), F32),
            jax.ShapeDtypeStruct((16, LANES), F32),
        ),
        in_specs=[hbm, hbm, hbm, hbm, pl.BlockSpec(memory_space=pltpu.SMEM), hbm, hbm],
        out_specs=(vmem,) * 3,
        scratch_shapes=[
            pltpu.VMEM((4, width, wide), BF16),
            pltpu.VMEM((4, width, wide), BF16),
            pltpu.VMEM((4, t_cols, LANES), BF16),
            pltpu.VMEM((4, t_cols, LANES), BF16),
            pltpu.VMEM((4, rows_q, q_width), BF16),
            pltpu.VMEM((4, rows_q, q_width), BF16),
            pltpu.VMEM((3, TILES, cut, LANES), BF16),
            pltpu.VMEM((3, TILES, rest, LANES), BF16),
            pltpu.VMEM((3, t_cols, LANES), BF16),
            pltpu.VMEM((2, 3, rows_q, q_half), BF16),
            pltpu.VMEM((TILES, cut, LANES), BF16),
            pltpu.VMEM((TILES, rest, LANES), BF16),
            pltpu.VMEM((t_cols, LANES), BF16),
            pltpu.VMEM((2, rows_q, q_half), BF16),
            pltpu.VMEM((TILES, cut, LANES), BF16),
            pltpu.VMEM((TILES, rest, LANES), BF16),
            pltpu.VMEM((TILES, cut, LANES), BF16),
            pltpu.VMEM((TILES, rest, LANES), BF16),
            pltpu.VMEM((2, t_cols, LANES), BF16),
            pltpu.VMEM((2, 2, rows_q, q_half), BF16),
            pltpu.VMEM((TILES, width, LANES), F32),
            pltpu.VMEM((width, LANES), BF16),
            pltpu.VMEM((t_cols, LANES), BF16),
            pltpu.VMEM((3, rows_q, q_width), BF16),
            pltpu.VMEM((width, LANES), F32),
            pltpu.VMEM((3, 8, LANES), F32),
            pltpu.VMEM((3, 8, LANES), F32),
            pltpu.VMEM((32, 5, LANES), F32),
            pltpu.VMEM((rows_d, width), F32),
            pltpu.VMEM((rows_q, q_width), F32),
            pltpu.VMEM((width,), F32),
            pltpu.SMEM((4,), F32),
            dma((6,)), dma((3,)), dma((12,)), dma((4,)), dma((10,)), dma((4,)), dma((2, TILES)), dma((2,)),
            dma, dma((3,)), dma((2,)), dma((4,)), dma((4,)),
            regular((3,)), regular((4,)), regular, regular((2,)), regular((2,)),
        ],
        compiler_params=pltpu.CompilerParams(
            collective_id=0, has_side_effects=True, vmem_limit_bytes=28 << 20),
    )(in_hbm(grad_rows), in_hbm(grad_query), in_hbm(down_moment), in_hbm(query_moment), step_count,
      in_hbm(down_second), in_hbm(query_second))

    return tuple(pl.pallas_call(
        finish,
        name="finish",
        out_shape=(
            jax.ShapeDtypeStruct((rows_d, width), F32),
            jax.ShapeDtypeStruct((rows_d, width), F32),
            jax.ShapeDtypeStruct((width,), F32),
            jax.ShapeDtypeStruct((rows_d, width), BF16),
            jax.ShapeDtypeStruct((rows_q, q_width), F32),
            jax.ShapeDtypeStruct((rows_q, q_width), F32),
            jax.ShapeDtypeStruct((4,), F32),
            jax.ShapeDtypeStruct((rows_q, q_width), BF16),
        ),
        in_specs=[vmem] * 5,
        out_specs=(hbm,) * 8,
        scratch_shapes=[
            pltpu.VMEM((rows_d, width), F32),
            pltpu.VMEM((rows_d, width), BF16),
            pltpu.VMEM((rows_q, q_width), F32),
            pltpu.VMEM((rows_q, q_width), BF16),
            pltpu.VMEM((width,), F32),
            pltpu.VMEM((4,), F32),
            dma((8,)),
        ],
        compiler_params=pltpu.CompilerParams(vmem_limit_bytes=24 << 20),
    )(n, m, q_m, down_param, query_param))


def solution(mesh):
    in_specs = (
        P("dp", "tensor", "ctx"),
        P("dp", "ctx", "tensor"),
        P(("tensor", "dp"), "ctx"),
        P(("tensor", "dp"), "ctx"),
        P("ctx"),
        P(("ctx", "dp"), "tensor"),
        P(("ctx", "dp"), "tensor"),
        P("tensor"),
        P(),
    )
    out_specs = (
        P(("tensor", "dp"), "ctx"),
        P(("tensor", "dp"), "ctx"),
        P("ctx"),
        P(("tensor", "dp"), "ctx"),
        P(("ctx", "dp"), "tensor"),
        P(("ctx", "dp"), "tensor"),
        P("tensor"),
        P(("ctx", "dp"), "tensor"),
    )
    body = functools.partial(shards, mesh.shape["ctx"])
    return jax.shard_map(body, mesh=mesh, in_specs=in_specs, out_specs=out_specs, check_vma=False)
```

```python
import functools
import math

import jax
import jax.numpy as jnp
from jax import lax
from jax.experimental import pallas as pl
from jax.experimental.pallas import tpu as pltpu
from jax.sharding import PartitionSpec as P

D = 4608
HEAD_DIM = 128
FF = 18432

BETA_ONE = 0.9
BETA_TWO = 0.95
EPSILON = 1e-08
LEARN_RATE = 0.003
DECAY_RATE = 0.1

MESH = pl.DeviceIdType.MESH
F32 = jnp.float32
BF16 = jnp.bfloat16

FAR, RIGHT, LEFT, SELF = range(4)
PLUS, MINUS = range(2)
LANES = 128
TILES = 4


def exchange(
    nz,
    gd, gq, dm, qm, steps, dsec, qsec,
    m_out, qm_out, n_out,
    own_d, prt_d, own_q, prt_q,
    snd_a, snd_b, snd_q, rly_a, rly_b, rly_q,
    fin_pa, fin_pb, fin_ma, fin_mb, fin_q,
    own_e, prt_e, snd_e, rly_e, fin_e, acc, stage_d, stage_q, tbuf, zbuf, zsend, dbuf, m_buf, qm_buf, dsec_v, qsec_v,
    own_sem, ds_sem, dr_sem, ss, rly_sem, fin_sem, join_sem, tsem, zs, zr, sums_sem, small_sem, stage_sem,
    hx, hz, rc, ry, rx, e_sem,
):
    div, rem = lax.div, lax.rem
    dp, tp, cp = lax.axis_index("dp"), lax.axis_index("tensor"), lax.axis_index("ctx")
    y, core = div(dp, 2), rem(dp, 2)
    cols_all, wide = own_d.shape[1], own_d.shape[2]
    cut = 2 * LANES
    rest = cols_all - cut
    extra = pl.ds(0, cols_all)
    pair = 2 * wide + LANES
    rows_q, q_cols = own_q.shape[1], own_q.shape[2]
    q_half = q_cols // 2
    at = {FAR: rem(y + 2, 4), RIGHT: rem(y + 1, 4), LEFT: rem(y + 3, 4), SELF: y}
    partner = y * 2 + (1 - core)
    after, before = rem(tp + 1, 4), rem(tp + 3, 4)

    def tell(sem, *device):
        pl.semaphore_signal(sem, inc=1, device_id=device, device_id_type=MESH)

    barrier = pltpu.get_barrier_semaphore()

    @pl.when(core == 1)
    def _():
        tell(barrier, partner, tp, cp)

    @pl.when(y < 3)
    def _():
        tell(barrier, dp + 2, tp, cp)

    @pl.when(y == 0)
    def _():
        tell(barrier, 6 + core, tp, cp)

    @pl.when(tp < 3)
    def _():
        tell(barrier, dp, tp + 1, cp)

    @pl.when(tp == 0)
    def _():
        tell(barrier, dp, 3, cp)

    @pl.when(cp < nz - 1)
    def _():
        tell(barrier, dp, tp, cp + 1)

    def one_if(test):
        return jnp.where(test, 1, 0)

    greeted = (1 - core) + one_if(y > 0) + one_if(y == 3) + one_if(tp > 0) + one_if(tp == 3) + one_if(cp > 0)

    span = {"A": (0, cut), "B": (cut, rest), "AB": (0, cols_all)}

    def main_piece(role, who, part, first, tiles):
        row, count = span[part]
        lanes = pl.multiple_of(at[role] * pair + who * (wide + LANES) + first * LANES, LANES)
        return gd.at[0, pl.ds(row, count), pl.ds(lanes, tiles * LANES)]

    def extra_piece(role):
        return gd.at[0, extra, pl.ds(pl.multiple_of(at[role] * pair + wide, LANES), LANES)]

    def query_piece(role, who):
        return gq.at[0, pl.ds(pl.multiple_of((at[role] * 2 + who) * rows_q, 8), rows_q), :]

    order = [(("q", FAR), 0), (("q", RIGHT), 1), (("q", LEFT), 1), (("d", FAR, "AB", 0, 1), 2)]
    order += [(("d", FAR, "AB", k, 1), 2 + k) for k in range(1, TILES)]
    order += [(("q", SELF), 9)]
    order += [(("d", RIGHT, "B", 0, TILES), 6), (("d", LEFT, "A", 0, TILES), 6)]
    order += [(("d", RIGHT, "A", 0, TILES), 7), (("d", LEFT, "B", 0, TILES), 7), (("d", SELF, "AB", 0, TILES), 8)]
    own_order = [(("q", FAR), 0), (("d", FAR, "AB", 0, TILES), 1)]
    own_rest = [(("q", role), 2) for role in (RIGHT, LEFT, SELF)]
    own_rest += [(("d", role, "AB", 0, TILES), 3) for role in (RIGHT, LEFT, SELF)]

    def piece(item, who):
        if item[0] == "q":
            return query_piece(item[1], who)
        return main_piece(item[1], who, *item[2:])

    def landing(item, d, q):
        if item[0] == "q":
            return q.at[item[1]]
        _, role, part, first, tiles = item
        row, count = span[part]
        return d.at[role, pl.ds(row, count), pl.ds(first * LANES, tiles * LANES)]

    def own_load(item, n):
        pltpu.make_async_copy(piece(item, core), landing(item, own_d, own_q), own_sem.at[n]).start()

    held = {("q", FAR): (stage_q.at[0], 0), ("q", RIGHT): (stage_q.at[1], 1), ("q", LEFT): (stage_q.at[2], 1),
            ("d", FAR, "AB", 0, 1): (stage_d, 2)}

    def stage_load(item):
        pltpu.make_async_copy(piece(item, 1 - core), held[item][0], stage_sem.at[held[item][1]]).start()

    stage_load(("q", FAR))
    own_load(*own_order[0])
    stage_load(("q", RIGHT))
    stage_load(("q", LEFT))
    stage_load(("d", FAR, "AB", 0, 1))
    own_load(*own_order[1])
    for entry in own_rest[:3]:
        own_load(*entry)

    def own_extra(role):
        pltpu.make_async_copy(extra_piece(role), own_e.at[role], e_sem.at[0 if role == FAR else 1]).start()

    @pl.when(core == 1)
    def _():
        own_extra(FAR)

    @pl.when(greeted > 0)
    def _():
        pl.semaphore_wait(barrier, greeted)

    @pl.when(core == 0)
    def _():
        tell(rc, partner, tp, cp)

    @pl.when(y > 0)
    def _():
        tell(ry.at[0], dp - 2, tp, cp)

    @pl.when(y == 3)
    def _():
        tell(ry.at[1], core, tp, cp)

    @pl.when(tp > 0)
    def _():
        tell(rx.at[0], dp, tp - 1, cp)

    @pl.when(tp == 3)
    def _():
        tell(rx.at[1], dp, 0, cp)

    @pl.when(cp > 0)
    def _():
        tell(hz.at[3], dp, tp, cp - 1)

    @pl.when(core == 1)
    def _():
        pl.semaphore_wait(rc, 1)

    kinds = {"q": 0, "d": 1}
    def settled(ref, sem):
        return pltpu.make_async_remote_copy(
            src_ref=ref, dst_ref=ref, send_sem=sem, recv_sem=sem, device_id=(partner, tp, cp), device_id_type=MESH)

    def prt_start(item, n):
        pltpu.make_async_remote_copy(
            src_ref=held[item][0] if item in held else piece(item, 1 - core), dst_ref=landing(item, prt_d, prt_q),
            send_sem=ds_sem.at[kinds[item[0]]], recv_sem=dr_sem.at[n],
            device_id=(partner, tp, cp), device_id_type=MESH).start()

    for n, item in enumerate(list(held)):
        if n != 2:
            ref = stage_q.at[pl.ds(1, 2)] if n == 1 else held[item][0]
            pltpu.make_async_copy(ref, ref, stage_sem.at[held[item][1]]).wait()
        prt_start(*order[n])
    def prt_extra(role):
        pltpu.make_async_remote_copy(
            src_ref=extra_piece(role), dst_ref=prt_e.at[role], send_sem=e_sem.at[2], recv_sem=e_sem.at[3 if role == FAR else 4],
            device_id=(partner, tp, cp), device_id_type=MESH).start()

    @pl.when(core == 0)
    def _():
        prt_extra(FAR)

    for entry in order[len(held):7]:
        prt_start(*entry)
    for entry in own_rest[3:]:
        own_load(*entry)
    @pl.when(core == 1)
    def _():
        for role in (LEFT, RIGHT, SELF):
            own_extra(role)

    @pl.when(core == 0)
    def _():
        for role in (LEFT, RIGHT, SELF):
            prt_extra(role)

    for entry in order[7:]:
        prt_start(*entry)

    small = [
        pltpu.make_async_copy(dsec, dsec_v, small_sem.at[0]),
        pltpu.make_async_copy(qsec, qsec_v, small_sem.at[1]),
        pltpu.make_async_copy(dm, m_buf, small_sem.at[2]),
        pltpu.make_async_copy(qm, qm_buf, small_sem.at[3]),
    ]
    for copy in small:
        copy.start()

    have = set()
    three = pl.ds(RIGHT, 3)
    own_ref = [own_q.at[FAR], own_d.at[FAR], own_q.at[three], own_d.at[three]]
    one_tile = prt_d.at[FAR, :, pl.ds(0, LANES)]
    prt_ref = [prt_q.at[FAR], prt_q.at[pl.ds(RIGHT, 2)]] + [one_tile] * 4 + [
        prt_d.at[RIGHT], prt_d.at[RIGHT], prt_d.at[SELF], prt_q.at[SELF]]

    def need(own, prt):
        if ("own", own) not in have:
            have.add(("own", own))
            pltpu.make_async_copy(own_ref[own], own_ref[own], own_sem.at[own]).wait()
        if ("prt", prt) not in have:
            have.add(("prt", prt))
            settled(prt_ref[prt], dr_sem.at[prt]).wait_recv()

    def main_sum(role, part, k):
        if role == FAR:
            need(1, 2 + k)
        elif role == SELF:
            need(3, 8)
        else:
            need(3, 6 if (role == RIGHT) == (part == "B") else 7)
        row, count = span[part]
        where = (role, pl.ds(row, count), pl.ds(k * LANES, LANES))
        return own_d[where].astype(F32) + prt_d[where].astype(F32)

    def query_sum(role, block):
        need(0, 0) if role == FAR else need(2, 9 if role == SELF else 1)
        where = (role, slice(None), pl.ds(block * q_half, q_half))
        return own_q[where].astype(F32) + prt_q[where].astype(F32)

    def y_send(way, value, src, send, dst, recv):
        src[...] = value.astype(BF16)
        pltpu.make_async_remote_copy(
            src_ref=src, dst_ref=dst, send_sem=ss.at[send], recv_sem=recv,
            device_id=((at[RIGHT] if way == PLUS else at[LEFT]) * 2 + core, tp, cp), device_id_type=MESH).start()

    def first_q():
        for way in (PLUS, MINUS):
            @pl.when(y < 3 if way == PLUS else y == 0)
            def _():
                pl.semaphore_wait(ry.at[way], 1)

            y_send(way, query_sum(FAR, way), snd_q.at[way, 0], 3, rly_q.at[way], rly_sem.at[9])

    def second_q():
        for way, role in ((PLUS, RIGHT), (MINUS, LEFT)):
            y_send(way, query_sum(role, 1 - way), snd_q.at[way, 1], 3, fin_q.at[way, 0], fin_sem.at[3])

    def third_q():
        settled(rly_q, rly_sem.at[9]).wait_recv()
        for way, role in ((PLUS, RIGHT), (MINUS, LEFT)):
            y_send(way, query_sum(role, way) + rly_q[way].astype(F32), snd_q.at[way, 2], 3, fin_q.at[way, 1], fin_sem.at[3])

    def extra_sum(role):
        return own_e[role].astype(F32) + prt_e[role].astype(F32)

    def extra_need(far):
        for buf, n in ((own_e, 0), (prt_e, 3)):
            ref = buf.at[FAR] if far else buf.at[three]
            settled(ref, e_sem.at[n if far else n + 1]).wait_recv()

    def first_e():
        @pl.when(core == 1)
        def _():
            extra_need(True)
            y_send(PLUS, extra_sum(FAR), snd_e.at[0], 4, rly_e, e_sem.at[5])

    def second_e():
        @pl.when(core == 1)
        def _():
            extra_need(False)
            y_send(MINUS, extra_sum(LEFT), snd_e.at[1], 4, fin_e.at[0], e_sem.at[6])

    def third_e():
        @pl.when(core == 1)
        def _():
            settled(rly_e, e_sem.at[5]).wait_recv()
            y_send(PLUS, extra_sum(RIGHT) + rly_e[...].astype(F32), snd_e.at[2], 4, fin_e.at[1], e_sem.at[6])

    def first_d(k):
        y_send(PLUS, main_sum(FAR, "A", k), snd_a.at[0, k], 0, rly_a.at[k], rly_sem.at[k])
        y_send(MINUS, main_sum(FAR, "B", k), snd_b.at[0, k], 1, rly_b.at[k], rly_sem.at[4 + k])

    def second_d(k):
        y_send(PLUS, main_sum(RIGHT, "B", k), snd_b.at[1, k], 1, fin_pb.at[k], fin_sem.at[0])
        y_send(MINUS, main_sum(LEFT, "A", k), snd_a.at[1, k], 0, fin_ma.at[k], fin_sem.at[1])

    def third_d(k):
        settled(rly_a.at[k], rly_sem.at[k]).wait_recv()
        y_send(PLUS, main_sum(RIGHT, "A", k) + rly_a[k].astype(F32), snd_a.at[2, k], 0, fin_pa.at[k], join_sem.at[PLUS, k])
        settled(rly_b.at[k], rly_sem.at[4 + k]).wait_recv()
        y_send(MINUS, main_sum(LEFT, "B", k) + rly_b[k].astype(F32), snd_b.at[2, k], 1, fin_mb.at[k], join_sem.at[MINUS, k])

    first_q()
    second_q()
    first_d(0)
    third_q()
    first_e()
    first_d(1)
    first_d(2)
    first_d(3)
    second_e()
    for k in range(TILES):
        second_d(k)
    third_e()

    @pl.when(cp < nz - 1)
    def _():
        pl.semaphore_wait(hz.at[3], 1)

    @pl.when(jnp.logical_and(cp > 0, cp < nz - 1))
    def _():
        tell(hz.at[0], dp, tp, cp - 1)
        tell(hz.at[1], dp, tp, cp + 1)

    for copy in small:
        copy.wait()

    def moment(old, mean):
        return BETA_ONE * old + (1.0 - BETA_ONE) * mean

    head_row = jnp.zeros((1, LANES), F32)
    lane = lax.broadcasted_iota(jnp.int32, (1, LANES), 1)
    settled(fin_q, fin_sem.at[3]).wait_recv()
    for block in (0, 1):
        mean = (query_sum(SELF, block) + fin_q[block, 1].astype(F32) + fin_q[1 - block, 0].astype(F32)) / 8
        where = (slice(None), pl.ds(block * q_half, q_half))
        qm_out[where] = moment(qm_buf[where], mean)
        square = jnp.sum(mean * mean, axis=0, keepdims=True)
        for h in range(2):
            part = jnp.sum(square[:, h * LANES:(h + 1) * LANES], axis=1, keepdims=True)
            head_row = jnp.where(lane == block * 2 + h, part, head_row)

    def z_copy(i):
        step = 1 << i
        peer = cp + step * (1 - 2 * rem(div(cp, step), 2))
        return pltpu.make_async_remote_copy(
            src_ref=zsend.at[i], dst_ref=zbuf.at[i], send_sem=zs, recv_sem=zr.at[i],
            device_id=(dp, tp, peer), device_id_type=MESH)

    z_copies = [z_copy(i) for i in range(3)]
    zsend[0] = jnp.broadcast_to(head_row, (8, LANES))
    z_copies[0].start()

    @pl.when(cp <= nz - 3)
    def _():
        pl.semaphore_wait(hz.at[0], 1)

    @pl.when(cp >= 2)
    def _():
        pl.semaphore_wait(hz.at[1], 1)

    @pl.when(jnp.logical_and(cp >= 2, cp <= nz - 3))
    def _():
        tell(hz.at[2], dp, tp, cp - 2)
        tell(hz.at[2], dp, tp, cp + 2)

    for k in range(TILES):
        third_d(k)
        if k % 2 == 1:
            i = (k + 1) // 2
            z_copies[i - 1].wait_recv()
            zsend[i] = zsend[i - 1] + zbuf[i - 1]
            if i == 2:
                pl.semaphore_wait(hz.at[2], 1)
            z_copies[i].start()

    settled(fin_ma, fin_sem.at[1]).wait_recv()
    settled(fin_pb, fin_sem.at[0]).wait_recv()
    for k in range(TILES):
        acc[k, pl.ds(0, cut), :] = main_sum(SELF, "A", k) + fin_ma[k].astype(F32)
        acc[k, pl.ds(cut, rest), :] = main_sum(SELF, "B", k) + fin_pb[k].astype(F32)
    for n, ref in enumerate((prt_q, prt_d)):
        settled(ref, ds_sem.at[n]).wait_send()

    swap_extra = pltpu.make_async_remote_copy(
        src_ref=tbuf.at[extra, :], dst_ref=tbuf.at[extra, :], send_sem=e_sem.at[7], recv_sem=e_sem.at[8],
        device_id=(partner, tp, cp), device_id_type=MESH)

    @pl.when(core == 1)
    def _():
        settled(fin_e, e_sem.at[6]).wait_recv()
        tbuf[extra, :] = (extra_sum(SELF) + fin_e[0].astype(F32) + fin_e[1].astype(F32)) / 8
        swap_extra.start()
        settled(snd_e, ss.at[4]).wait_send()

    @pl.when(core == 0)
    def _():
        settled(prt_e, e_sem.at[2]).wait_send()

    @pl.when(tp < 3)
    def _():
        pl.semaphore_wait(rx.at[0], 1)

    @pl.when(tp == 0)
    def _():
        pl.semaphore_wait(rx.at[1], 1)

    tell(hx.at[0], dp, before, cp)
    tell(hx.at[1], dp, after, cp)
    settled(snd_q, ss.at[3]).wait_send()

    def column_squares(rows):
        return jnp.sum(rows * rows, axis=0, keepdims=True)

    sums_a, sums_b = jnp.zeros((1, cut), F32), jnp.zeros((1, rest), F32)
    for k in range(TILES):
        if k == 1:
            pl.semaphore_wait(hx.at[0], 1)
            pl.semaphore_wait(hx.at[1], 1)
            tell(hx.at[2], dp, after, cp)
            @pl.when(core == 0)
            def _():
                swap_extra.wait_recv()

            both = jnp.transpose(tbuf[...])
            own_rows = jnp.where(core == 0, both[:LANES // 2], both[LANES // 2:])
            there = pl.ds(pl.multiple_of((1 - core) * wide, LANES // 2), LANES // 2)
            m_out[there, :] = moment(m_buf[there, :], own_rows)
            sums_a = sums_a + column_squares(own_rows[:, :cut])
            sums_b = sums_b + column_squares(own_rows[:, cut:])
        here = pl.ds(pl.multiple_of(core * (LANES // 2) + k * LANES, LANES // 2), LANES)
        settled(fin_pa.at[k], join_sem.at[PLUS, k]).wait_recv()
        rows_a = jnp.transpose((acc[k, pl.ds(0, cut), :] + fin_pa[k].astype(F32)) / 8)
        settled(fin_mb.at[k], join_sem.at[MINUS, k]).wait_recv()
        rows_b = jnp.transpose((acc[k, pl.ds(cut, rest), :] + fin_mb[k].astype(F32)) / 8)
        sums_a = sums_a + column_squares(rows_a)
        sums_b = sums_b + column_squares(rows_b)
        if k < TILES - 1:
            m_out[here, pl.ds(0, cut)] = moment(m_buf[here, pl.ds(0, cut)], rows_a)
            m_out[here, pl.ds(cut, rest)] = moment(m_buf[here, pl.ds(cut, rest)], rows_b)
        else:
            m_out[here, pl.ds(0, cut)] = rows_a
            m_out[here, pl.ds(cut, rest)] = rows_b

    z_copies[2].wait_recv()
    head_sum = zsend[2, pl.ds(0, 1), :] + zbuf[2, pl.ds(0, 1), :]

    slot = tp * 8 + dp
    mine = dbuf.at[slot]
    mine[pl.ds(0, 1), :] = sums_a[:, :LANES]
    mine[pl.ds(1, 1), :] = sums_a[:, LANES:]
    mine[pl.ds(2, 1), :] = sums_b[:, :LANES]
    mine[pl.ds(3, 1), :] = sums_b[:, LANES:2 * LANES]
    mine[pl.ds(4, 1), :] = jnp.concatenate([sums_b[:, 2 * LANES:], head_sum[:, :LANES // 2]], axis=1)
    pl.semaphore_wait(hx.at[2], 1)

    others = [(k, j) for k in (2, 1, 3, 0) for j in (4, 5, 2, 3, 6, 7, 1, 0) if (k, j) != (0, 0)]
    for k, j in others:
        pltpu.make_async_remote_copy(
            src_ref=mine, dst_ref=mine, send_sem=sums_sem.at[0], recv_sem=sums_sem.at[1],
            device_id=(rem(dp + j, 8), rem(tp + k, 4), cp), device_id_type=MESH).start()

    here = pl.ds(pl.multiple_of(core * (LANES // 2) + (TILES - 1) * LANES, LANES // 2), LANES)
    m_out[here, :] = moment(m_buf[here, :], m_out[here, :])
    step = jnp.full((1, LANES), steps[0], jnp.int32).astype(F32)
    keep_one = 1.0 - jnp.exp(step * math.log(BETA_ONE))
    keep_two = 1.0 - jnp.exp(step * math.log(BETA_TWO))
    n_out[...] = jnp.zeros(n_out.shape, F32)

    settled(snd_a, ss.at[0]).wait_send()
    settled(snd_b, ss.at[1]).wait_send()
    @pl.when(core == 1)
    def _():
        swap_extra.wait_send()

    settled(zsend, zs).wait_send()
    everyone_else = dbuf.at[pl.ds(0, len(others))]
    settled(everyone_else, sums_sem.at[0]).wait_send()
    settled(everyone_else, sums_sem.at[1]).wait_recv()

    def total(column):
        found = dbuf[column * 8]
        for p in range(1, 8):
            found = found + dbuf[column * 8 + p]
        return found

    whole = (total(0) + total(1)) + (total(2) + total(3))
    part = pltpu.roll(total(tp)[4:5, :], LANES // 2, 1)

    def advance(old, mean, n):
        new = BETA_TWO * old + (1.0 - BETA_TWO) * mean
        n_out[n:n + 1, :] = 1.0 / (keep_one * (jnp.sqrt(new / keep_two) + EPSILON))
        n_out[n + 8:n + 9, :] = new

    for k in range(5):
        if k < 4:
            old = dsec_v[pl.ds(k * LANES, LANES)].reshape(1, LANES)
        else:
            old = dsec_v[pl.ds(k * LANES, LANES // 2)].reshape(1, LANES // 2)
            old = jnp.concatenate([old, jnp.ones((1, LANES // 2), F32)], axis=1)
        advance(old, whole[k:k + 1, :] / FF, k)
    old = jnp.ones((1, LANES), F32)
    for h in range(4):
        old = jnp.where(lane == h, qsec_v[h], old)
    advance(old, part / (D * HEAD_DIM), 5)


def finish(
    n_in, m_in, qm_in, dp_in, qp_in,
    dp_out, dm_out, ds_out, du_out, qp_out, qm_out, qs_out, qu_out,
    po_buf, uo_buf, qpo, quo, ds_buf, qs_buf, out_sem,
):
    rows_d, width = dp_in.shape

    def store(n, src, dst):
        pltpu.make_async_copy(src, dst, out_sem.at[n]).start()

    def update(param, moment, scale):
        step = moment * scale
        param_new = param - LEARN_RATE * (step + DECAY_RATE * param)
        return param_new, step.astype(BF16)

    block = rows_d // 4
    store(0, m_in, dm_out)
    for k in range(5):
        count = LANES if k < 4 else width - 4 * LANES
        ds_buf[pl.ds(k * LANES, count)] = n_in[8 + k:9 + k, :count].reshape(count)
    qs_buf[...] = n_in[13:14, :4].reshape(4)
    store(1, ds_buf, ds_out)
    store(2, qs_buf, qs_out)
    for b in range(4):
        rows = pl.ds(b * block, block)
        for k in range(5):
            lanes = pl.ds(k * LANES, LANES if k < 4 else width - 4 * LANES)
            po_buf[rows, lanes], uo_buf[rows, lanes] = update(
                dp_in[rows, lanes], m_in[rows, lanes], n_in[k:k + 1, :lanes.size])
        store(3, po_buf.at[rows, :], dp_out.at[rows, :])
        store(4, uo_buf.at[rows, :], du_out.at[rows, :])
        if b == 0:
            store(5, qm_in, qm_out)
    for h in range(4):
        lanes = pl.ds(h * LANES, LANES)
        qpo[:, lanes], quo[:, lanes] = update(qp_in[:, lanes], qm_in[:, lanes], n_in[5:6, h:h + 1])
    store(6, qpo, qp_out)
    store(7, quo, qu_out)
    for n, (src, dst) in enumerate((
            (m_in, dm_out), (ds_buf, ds_out), (qs_buf, qs_out), (po_buf, dp_out), (uo_buf, du_out),
            (qm_in, qm_out), (qpo, qp_out), (quo, qu_out))):
        pltpu.make_async_copy(src, dst, out_sem.at[n]).wait()


def shards(nz, grad_down, grad_query, down_param, down_moment, down_second,
           query_param, query_moment, query_second, step_count):
    rows_d, width = down_param.shape
    rows_q, q_width = query_param.shape
    cut, wide = 2 * LANES, TILES * LANES
    rest, t_cols, q_half = width - cut, width, q_width // 2
    hbm = pl.BlockSpec(memory_space=pltpu.HBM)
    vmem = pl.BlockSpec(memory_space=pltpu.VMEM)
    dma = pltpu.SemaphoreType.DMA
    regular = pltpu.SemaphoreType.REGULAR
    grad_rows = jnp.swapaxes(grad_down, 1, 2)
    in_hbm = lambda x: pltpu.with_memory_space_constraint(x, pltpu.HBM)
    m, q_m, n = pl.pallas_call(
        functools.partial(exchange, nz),
        name="exchange",
        out_shape=(
            jax.ShapeDtypeStruct((rows_d, width), F32),
            jax.ShapeDtypeStruct((rows_q, q_width), F32),
            jax.ShapeDtypeStruct((16, LANES), F32),
        ),
        in_specs=[hbm, hbm, hbm, hbm, pl.BlockSpec(memory_space=pltpu.SMEM), hbm, hbm],
        out_specs=(vmem,) * 3,
        scratch_shapes=[
            pltpu.VMEM((4, width, wide), BF16),
            pltpu.VMEM((4, width, wide), BF16),
            pltpu.VMEM((4, rows_q, q_width), BF16),
            pltpu.VMEM((4, rows_q, q_width), BF16),
            pltpu.VMEM((3, TILES, cut, LANES), BF16),
            pltpu.VMEM((3, TILES, rest, LANES), BF16),
            pltpu.VMEM((2, 3, rows_q, q_half), BF16),
            pltpu.VMEM((TILES, cut, LANES), BF16),
            pltpu.VMEM((TILES, rest, LANES), BF16),
            pltpu.VMEM((2, rows_q, q_half), BF16),
            pltpu.VMEM((TILES, cut, LANES), BF16),
            pltpu.VMEM((TILES, rest, LANES), BF16),
            pltpu.VMEM((TILES, cut, LANES), BF16),
            pltpu.VMEM((TILES, rest, LANES), BF16),
            pltpu.VMEM((2, 2, rows_q, q_half), BF16),
            pltpu.VMEM((4, t_cols, LANES), BF16),
            pltpu.VMEM((4, t_cols, LANES), BF16),
            pltpu.VMEM((3, t_cols, LANES), BF16),
            pltpu.VMEM((t_cols, LANES), BF16),
            pltpu.VMEM((2, t_cols, LANES), BF16),
            pltpu.VMEM((TILES, width, LANES), F32),
            pltpu.VMEM((width, LANES), BF16),
            pltpu.VMEM((3, rows_q, q_width), BF16),
            pltpu.VMEM((width, LANES), F32),
            pltpu.VMEM((3, 8, LANES), F32),
            pltpu.VMEM((3, 8, LANES), F32),
            pltpu.VMEM((32, 5, LANES), F32),
            pltpu.VMEM((rows_d, width), F32),
            pltpu.VMEM((rows_q, q_width), F32),
            pltpu.VMEM((width,), F32),
            pltpu.SMEM((4,), F32),
            dma((6,)), dma((3,)), dma((12,)), dma((5,)), dma((10,)), dma((4,)), dma((2, TILES)), dma((2,)),
            dma, dma((3,)), dma((2,)), dma((4,)), dma((4,)),
            regular((3,)), regular((4,)), regular, regular((2,)), regular((2,)), dma((9,)),
        ],
        compiler_params=pltpu.CompilerParams(
            collective_id=0, has_side_effects=True, vmem_limit_bytes=28 << 20),
    )(in_hbm(grad_rows), in_hbm(grad_query), in_hbm(down_moment), in_hbm(query_moment), step_count,
      in_hbm(down_second), in_hbm(query_second))

    return tuple(pl.pallas_call(
        finish,
        name="finish",
        out_shape=(
            jax.ShapeDtypeStruct((rows_d, width), F32),
            jax.ShapeDtypeStruct((rows_d, width), F32),
            jax.ShapeDtypeStruct((width,), F32),
            jax.ShapeDtypeStruct((rows_d, width), BF16),
            jax.ShapeDtypeStruct((rows_q, q_width), F32),
            jax.ShapeDtypeStruct((rows_q, q_width), F32),
            jax.ShapeDtypeStruct((4,), F32),
            jax.ShapeDtypeStruct((rows_q, q_width), BF16),
        ),
        in_specs=[vmem] * 5,
        out_specs=(hbm,) * 8,
        scratch_shapes=[
            pltpu.VMEM((rows_d, width), F32),
            pltpu.VMEM((rows_d, width), BF16),
            pltpu.VMEM((rows_q, q_width), F32),
            pltpu.VMEM((rows_q, q_width), BF16),
            pltpu.VMEM((width,), F32),
            pltpu.VMEM((4,), F32),
            dma((8,)),
        ],
        compiler_params=pltpu.CompilerParams(vmem_limit_bytes=24 << 20),
    )(n, m, q_m, down_param, query_param))


def solution(mesh):
    in_specs = (
        P("dp", "tensor", "ctx"),
        P("dp", "ctx", "tensor"),
        P(("tensor", "dp"), "ctx"),
        P(("tensor", "dp"), "ctx"),
        P("ctx"),
        P(("ctx", "dp"), "tensor"),
        P(("ctx", "dp"), "tensor"),
        P("tensor"),
        P(),
    )
    out_specs = (
        P(("tensor", "dp"), "ctx"),
        P(("tensor", "dp"), "ctx"),
        P("ctx"),
        P(("tensor", "dp"), "ctx"),
        P(("ctx", "dp"), "tensor"),
        P(("ctx", "dp"), "tensor"),
        P("tensor"),
        P(("ctx", "dp"), "tensor"),
    )
    body = functools.partial(shards, mesh.shape["ctx"])
    return jax.shard_map(body, mesh=mesh, in_specs=in_specs, out_specs=out_specs, check_vma=False)
```

```python
import functools
import math

import jax
import jax.numpy as jnp
from jax import lax
from jax.experimental import pallas as pl
from jax.experimental.pallas import tpu as pltpu
from jax.sharding import PartitionSpec as P

D = 4608
HEAD_DIM = 128
FF = 18432

BETA_ONE = 0.9
BETA_TWO = 0.95
EPSILON = 1e-08
LEARN_RATE = 0.003
DECAY_RATE = 0.1

MESH = pl.DeviceIdType.MESH
F32 = jnp.float32
BF16 = jnp.bfloat16

FAR, RIGHT, LEFT, SELF = range(4)
PLUS, MINUS = range(2)
LANES = 128
TILES = 4


def exchange(
    nz,
    gd, gq, dm, qm, steps, dsec, qsec,
    m_out, qm_out, n_out,
    own_d, prt_d, own_q, prt_q,
    snd_a, snd_b, snd_q, rly_a, rly_b, rly_q,
    fin_pa, fin_pb, fin_ma, fin_mb, fin_q,
    own_e, prt_e, snd_e, rly_e, fin_e, acc, stage_d, stage_q, tbuf, zbuf, zsend, dbuf, m_buf, qm_buf, dsec_v, qsec_v,
    own_sem, ds_sem, dr_sem, ss, rly_sem, fin_sem, join_sem, tsem, zs, zr, sums_sem, small_sem, stage_sem,
    hx, hz, rc, ry, rx, e_sem,
):
    div, rem = lax.div, lax.rem
    dp, tp, cp = lax.axis_index("dp"), lax.axis_index("tensor"), lax.axis_index("ctx")
    y, core = div(dp, 2), rem(dp, 2)
    cols_all, wide = own_d.shape[1], own_d.shape[2]
    cut = 2 * LANES
    rest = cols_all - cut
    extra = pl.ds(0, cols_all)
    pair = 2 * wide + LANES
    rows_q, q_cols = own_q.shape[1], own_q.shape[2]
    q_half = q_cols // 2
    at = {FAR: rem(y + 2, 4), RIGHT: rem(y + 1, 4), LEFT: rem(y + 3, 4), SELF: y}
    partner = y * 2 + (1 - core)
    after, before = rem(tp + 1, 4), rem(tp + 3, 4)

    def tell(sem, *device):
        pl.semaphore_signal(sem, inc=1, device_id=device, device_id_type=MESH)

    barrier = pltpu.get_barrier_semaphore()

    @pl.when(core == 1)
    def _():
        tell(barrier, partner, tp, cp)

    @pl.when(y < 3)
    def _():
        tell(barrier, dp + 2, tp, cp)

    @pl.when(y == 0)
    def _():
        tell(barrier, 6 + core, tp, cp)

    @pl.when(tp < 3)
    def _():
        tell(barrier, dp, tp + 1, cp)

    @pl.when(tp == 0)
    def _():
        tell(barrier, dp, 3, cp)

    @pl.when(cp < nz - 1)
    def _():
        tell(barrier, dp, tp, cp + 1)

    def one_if(test):
        return jnp.where(test, 1, 0)

    greeted = (1 - core) + one_if(y > 0) + one_if(y == 3) + one_if(tp > 0) + one_if(tp == 3) + one_if(cp > 0)

    span = {"A": (0, cut), "B": (cut, rest), "AB": (0, cols_all)}

    def main_piece(role, who, part, first, tiles):
        row, count = span[part]
        lanes = pl.multiple_of(at[role] * pair + who * (wide + LANES) + first * LANES, LANES)
        return gd.at[0, pl.ds(row, count), pl.ds(lanes, tiles * LANES)]

    def extra_piece(role):
        return gd.at[0, extra, pl.ds(pl.multiple_of(at[role] * pair + wide, LANES), LANES)]

    def query_piece(role, who):
        return gq.at[0, pl.ds(pl.multiple_of((at[role] * 2 + who) * rows_q, 8), rows_q), :]

    order = [(("q", FAR), 0), (("q", RIGHT), 1), (("q", LEFT), 1), (("d", FAR, "AB", 0, 1), 2)]
    order += [(("d", FAR, "AB", k, 1), 2 + k) for k in range(1, TILES)]
    order += [(("q", SELF), 9)]
    order += [(("d", RIGHT, "B", 0, TILES), 6), (("d", LEFT, "A", 0, TILES), 6)]
    order += [(("d", RIGHT, "A", 0, TILES), 7), (("d", LEFT, "B", 0, TILES), 7), (("d", SELF, "AB", 0, TILES), 8)]
    own_order = [(("q", FAR), 0), (("d", FAR, "AB", 0, TILES), 1)]
    own_rest = [(("q", role), 2) for role in (RIGHT, LEFT, SELF)]
    own_rest += [(("d", role, "AB", 0, TILES), 3) for role in (RIGHT, LEFT, SELF)]

    def piece(item, who):
        if item[0] == "q":
            return query_piece(item[1], who)
        return main_piece(item[1], who, *item[2:])

    def landing(item, d, q):
        if item[0] == "q":
            return q.at[item[1]]
        _, role, part, first, tiles = item
        row, count = span[part]
        return d.at[role, pl.ds(row, count), pl.ds(first * LANES, tiles * LANES)]

    def own_load(item, n):
        pltpu.make_async_copy(piece(item, core), landing(item, own_d, own_q), own_sem.at[n]).start()

    held = {("q", FAR): (stage_q.at[0], 0), ("q", RIGHT): (stage_q.at[1], 1), ("q", LEFT): (stage_q.at[2], 1),
            ("d", FAR, "AB", 0, 1): (stage_d, 2)}

    def stage_load(item):
        pltpu.make_async_copy(piece(item, 1 - core), held[item][0], stage_sem.at[held[item][1]]).start()

    stage_load(("q", FAR))
    own_load(*own_order[0])
    stage_load(("q", RIGHT))
    stage_load(("q", LEFT))
    stage_load(("d", FAR, "AB", 0, 1))
    own_load(*own_order[1])
    for entry in own_rest[:3]:
        own_load(*entry)

    def own_extra(role):
        pltpu.make_async_copy(extra_piece(role), own_e.at[role], e_sem.at[0 if role == FAR else 1]).start()

    @pl.when(core == 1)
    def _():
        own_extra(FAR)

    @pl.when(greeted > 0)
    def _():
        pl.semaphore_wait(barrier, greeted)

    @pl.when(core == 0)
    def _():
        tell(rc, partner, tp, cp)

    @pl.when(y > 0)
    def _():
        tell(ry.at[0], dp - 2, tp, cp)

    @pl.when(y == 3)
    def _():
        tell(ry.at[1], core, tp, cp)

    @pl.when(tp > 0)
    def _():
        tell(rx.at[0], dp, tp - 1, cp)

    @pl.when(tp == 3)
    def _():
        tell(rx.at[1], dp, 0, cp)

    @pl.when(cp > 0)
    def _():
        tell(hz.at[3], dp, tp, cp - 1)

    @pl.when(core == 1)
    def _():
        pl.semaphore_wait(rc, 1)

    kinds = {"q": 0, "d": 1}
    def settled(ref, sem):
        return pltpu.make_async_remote_copy(
            src_ref=ref, dst_ref=ref, send_sem=sem, recv_sem=sem, device_id=(partner, tp, cp), device_id_type=MESH)

    def prt_start(item, n):
        pltpu.make_async_remote_copy(
            src_ref=held[item][0] if item in held else piece(item, 1 - core), dst_ref=landing(item, prt_d, prt_q),
            send_sem=ds_sem.at[kinds[item[0]]], recv_sem=dr_sem.at[n],
            device_id=(partner, tp, cp), device_id_type=MESH).start()

    for n, item in enumerate(list(held)):
        if n != 2:
            ref = stage_q.at[pl.ds(1, 2)] if n == 1 else held[item][0]
            pltpu.make_async_copy(ref, ref, stage_sem.at[held[item][1]]).wait()
        prt_start(*order[n])
    def prt_extra(role):
        pltpu.make_async_remote_copy(
            src_ref=extra_piece(role), dst_ref=prt_e.at[role], send_sem=e_sem.at[2], recv_sem=e_sem.at[3 if role == FAR else 4],
            device_id=(partner, tp, cp), device_id_type=MESH).start()

    @pl.when(core == 0)
    def _():
        prt_extra(FAR)

    for entry in order[len(held):7]:
        prt_start(*entry)
    for entry in own_rest[3:]:
        own_load(*entry)
    @pl.when(core == 1)
    def _():
        for role in (LEFT, RIGHT, SELF):
            own_extra(role)

    @pl.when(core == 0)
    def _():
        for role in (LEFT, RIGHT, SELF):
            prt_extra(role)

    for entry in order[7:]:
        prt_start(*entry)

    small = [
        pltpu.make_async_copy(dsec, dsec_v, small_sem.at[0]),
        pltpu.make_async_copy(qsec, qsec_v, small_sem.at[1]),
        pltpu.make_async_copy(dm, m_buf, small_sem.at[2]),
        pltpu.make_async_copy(qm, qm_buf, small_sem.at[3]),
    ]
    for copy in small:
        copy.start()

    have = set()
    three = pl.ds(RIGHT, 3)
    own_ref = [own_q.at[FAR], own_d.at[FAR], own_q.at[three], own_d.at[three]]
    one_tile = prt_d.at[FAR, :, pl.ds(0, LANES)]
    prt_ref = [prt_q.at[FAR], prt_q.at[pl.ds(RIGHT, 2)]] + [one_tile] * 4 + [
        prt_d.at[RIGHT], prt_d.at[RIGHT], prt_d.at[SELF], prt_q.at[SELF]]

    def need(own, prt):
        if ("own", own) not in have:
            have.add(("own", own))
            pltpu.make_async_copy(own_ref[own], own_ref[own], own_sem.at[own]).wait()
        if ("prt", prt) not in have:
            have.add(("prt", prt))
            settled(prt_ref[prt], dr_sem.at[prt]).wait_recv()

    def main_sum(role, part, k):
        if role == FAR:
            need(1, 2 + k)
        elif role == SELF:
            need(3, 8)
        else:
            need(3, 6 if (role == RIGHT) == (part == "B") else 7)
        row, count = span[part]
        where = (role, pl.ds(row, count), pl.ds(k * LANES, LANES))
        return own_d[where].astype(F32) + prt_d[where].astype(F32)

    def query_sum(role, block):
        need(0, 0) if role == FAR else need(2, 9 if role == SELF else 1)
        where = (role, slice(None), pl.ds(block * q_half, q_half))
        return own_q[where].astype(F32) + prt_q[where].astype(F32)

    def y_send(way, value, src, send, dst, recv):
        src[...] = value.astype(BF16)
        pltpu.make_async_remote_copy(
            src_ref=src, dst_ref=dst, send_sem=ss.at[send], recv_sem=recv,
            device_id=((at[RIGHT] if way == PLUS else at[LEFT]) * 2 + core, tp, cp), device_id_type=MESH).start()

    def first_q():
        for way in (PLUS, MINUS):
            @pl.when(y < 3 if way == PLUS else y == 0)
            def _():
                pl.semaphore_wait(ry.at[way], 1)

            y_send(way, query_sum(FAR, way), snd_q.at[way, 0], 3, rly_q.at[way], rly_sem.at[9])

    def second_q():
        for way, role in ((PLUS, RIGHT), (MINUS, LEFT)):
            y_send(way, query_sum(role, 1 - way), snd_q.at[way, 1], 3, fin_q.at[way, 0], fin_sem.at[3])

    def third_q():
        settled(rly_q, rly_sem.at[9]).wait_recv()
        for way, role in ((PLUS, RIGHT), (MINUS, LEFT)):
            y_send(way, query_sum(role, way) + rly_q[way].astype(F32), snd_q.at[way, 2], 3, fin_q.at[way, 1], fin_sem.at[3])

    def extra_sum(role):
        return own_e[role].astype(F32) + prt_e[role].astype(F32)

    def extra_need(far):
        for buf, n in ((own_e, 0), (prt_e, 3)):
            ref = buf.at[FAR] if far else buf.at[three]
            settled(ref, e_sem.at[n if far else n + 1]).wait_recv()

    def first_e():
        @pl.when(core == 1)
        def _():
            extra_need(True)
            y_send(PLUS, extra_sum(FAR), snd_e.at[0], 4, rly_e, e_sem.at[5])

    def second_e():
        @pl.when(core == 1)
        def _():
            extra_need(False)
            y_send(MINUS, extra_sum(LEFT), snd_e.at[1], 4, fin_e.at[0], e_sem.at[6])

    def third_e():
        @pl.when(core == 1)
        def _():
            settled(rly_e, e_sem.at[5]).wait_recv()
            y_send(PLUS, extra_sum(RIGHT) + rly_e[...].astype(F32), snd_e.at[2], 4, fin_e.at[1], e_sem.at[6])

    def first_d(k):
        y_send(PLUS, main_sum(FAR, "A", k), snd_a.at[0, k], 0, rly_a.at[k], rly_sem.at[k])
        y_send(MINUS, main_sum(FAR, "B", k), snd_b.at[0, k], 1, rly_b.at[k], rly_sem.at[4 + k])

    def second_d(k):
        y_send(PLUS, main_sum(RIGHT, "B", k), snd_b.at[1, k], 1, fin_pb.at[k], fin_sem.at[0])
        y_send(MINUS, main_sum(LEFT, "A", k), snd_a.at[1, k], 0, fin_ma.at[k], fin_sem.at[1])

    def third_d(k):
        settled(rly_a.at[k], rly_sem.at[k]).wait_recv()
        y_send(PLUS, main_sum(RIGHT, "A", k) + rly_a[k].astype(F32), snd_a.at[2, k], 0, fin_pa.at[k], join_sem.at[PLUS, k])
        settled(rly_b.at[k], rly_sem.at[4 + k]).wait_recv()
        y_send(MINUS, main_sum(LEFT, "B", k) + rly_b[k].astype(F32), snd_b.at[2, k], 1, fin_mb.at[k], join_sem.at[MINUS, k])

    first_q()
    second_q()
    first_d(0)
    third_q()
    first_e()
    first_d(1)
    first_d(2)
    first_d(3)
    second_e()
    for k in range(TILES):
        second_d(k)
    third_e()

    @pl.when(cp < nz - 1)
    def _():
        pl.semaphore_wait(hz.at[3], 1)

    @pl.when(jnp.logical_and(cp > 0, cp < nz - 1))
    def _():
        tell(hz.at[0], dp, tp, cp - 1)
        tell(hz.at[1], dp, tp, cp + 1)

    for copy in small:
        copy.wait()

    def moment(old, mean):
        return BETA_ONE * old + (1.0 - BETA_ONE) * mean

    head_row = jnp.zeros((1, LANES), F32)
    lane = lax.broadcasted_iota(jnp.int32, (1, LANES), 1)
    settled(fin_q, fin_sem.at[3]).wait_recv()
    for block in (0, 1):
        mean = (query_sum(SELF, block) + fin_q[block, 1].astype(F32) + fin_q[1 - block, 0].astype(F32)) / 8
        where = (slice(None), pl.ds(block * q_half, q_half))
        qm_out[where] = moment(qm_buf[where], mean)
        square = jnp.sum(mean * mean, axis=0, keepdims=True)
        for h in range(2):
            part = jnp.sum(square[:, h * LANES:(h + 1) * LANES], axis=1, keepdims=True)
            head_row = jnp.where(lane == block * 2 + h, part, head_row)

    def z_copy(i):
        step = 1 << i
        peer = cp + step * (1 - 2 * rem(div(cp, step), 2))
        return pltpu.make_async_remote_copy(
            src_ref=zsend.at[i], dst_ref=zbuf.at[i], send_sem=zs, recv_sem=zr.at[i],
            device_id=(dp, tp, peer), device_id_type=MESH)

    z_copies = [z_copy(i) for i in range(3)]
    zsend[0] = jnp.broadcast_to(head_row, (8, LANES))
    z_copies[0].start()

    @pl.when(cp <= nz - 3)
    def _():
        pl.semaphore_wait(hz.at[0], 1)

    @pl.when(cp >= 2)
    def _():
        pl.semaphore_wait(hz.at[1], 1)

    @pl.when(jnp.logical_and(cp >= 2, cp <= nz - 3))
    def _():
        tell(hz.at[2], dp, tp, cp - 2)
        tell(hz.at[2], dp, tp, cp + 2)

    for k in range(TILES):
        third_d(k)
        if k % 2 == 1:
            i = (k + 1) // 2
            z_copies[i - 1].wait_recv()
            zsend[i] = zsend[i - 1] + zbuf[i - 1]
            if i == 2:
                pl.semaphore_wait(hz.at[2], 1)
            z_copies[i].start()

    settled(fin_ma, fin_sem.at[1]).wait_recv()
    settled(fin_pb, fin_sem.at[0]).wait_recv()
    for k in range(TILES):
        acc[k, pl.ds(0, cut), :] = main_sum(SELF, "A", k) + fin_ma[k].astype(F32)
        acc[k, pl.ds(cut, rest), :] = main_sum(SELF, "B", k) + fin_pb[k].astype(F32)
    for n, ref in enumerate((prt_q, prt_d)):
        settled(ref, ds_sem.at[n]).wait_send()

    swap_extra = pltpu.make_async_remote_copy(
        src_ref=tbuf.at[extra, :], dst_ref=tbuf.at[extra, :], send_sem=e_sem.at[7], recv_sem=e_sem.at[8],
        device_id=(partner, tp, cp), device_id_type=MESH)

    @pl.when(core == 1)
    def _():
        settled(fin_e, e_sem.at[6]).wait_recv()
        tbuf[extra, :] = (extra_sum(SELF) + fin_e[0].astype(F32) + fin_e[1].astype(F32)) / 8
        swap_extra.start()
        settled(snd_e, ss.at[4]).wait_send()

    @pl.when(core == 0)
    def _():
        settled(prt_e, e_sem.at[2]).wait_send()

    @pl.when(tp < 3)
    def _():
        pl.semaphore_wait(rx.at[0], 1)

    @pl.when(tp == 0)
    def _():
        pl.semaphore_wait(rx.at[1], 1)

    tell(hx.at[0], dp, before, cp)
    tell(hx.at[1], dp, after, cp)
    settled(snd_q, ss.at[3]).wait_send()

    def column_squares(rows):
        return jnp.sum(rows * rows, axis=0, keepdims=True)

    sums_a, sums_b = jnp.zeros((1, cut), F32), jnp.zeros((1, rest), F32)
    for k in range(TILES):
        if k == 1:
            pl.semaphore_wait(hx.at[0], 1)
            pl.semaphore_wait(hx.at[1], 1)
            tell(hx.at[2], dp, after, cp)
            @pl.when(core == 0)
            def _():
                swap_extra.wait_recv()

            both = jnp.transpose(tbuf[...])
            own_rows = jnp.where(core == 0, both[:LANES // 2], both[LANES // 2:])
            there = pl.ds(pl.multiple_of((1 - core) * wide, LANES // 2), LANES // 2)
            m_out[there, :] = moment(m_buf[there, :], own_rows)
            sums_a = sums_a + column_squares(own_rows[:, :cut])
            sums_b = sums_b + column_squares(own_rows[:, cut:])
        here = pl.ds(pl.multiple_of(core * (LANES // 2) + k * LANES, LANES // 2), LANES)
        settled(fin_pa.at[k], join_sem.at[PLUS, k]).wait_recv()
        rows_a = jnp.transpose((acc[k, pl.ds(0, cut), :] + fin_pa[k].astype(F32)) / 8)
        settled(fin_mb.at[k], join_sem.at[MINUS, k]).wait_recv()
        rows_b = jnp.transpose((acc[k, pl.ds(cut, rest), :] + fin_mb[k].astype(F32)) / 8)
        sums_a = sums_a + column_squares(rows_a)
        sums_b = sums_b + column_squares(rows_b)
        if k < TILES - 1:
            m_out[here, pl.ds(0, cut)] = moment(m_buf[here, pl.ds(0, cut)], rows_a)
            m_out[here, pl.ds(cut, rest)] = moment(m_buf[here, pl.ds(cut, rest)], rows_b)
        else:
            m_out[here, pl.ds(0, cut)] = rows_a
            m_out[here, pl.ds(cut, rest)] = rows_b

    z_copies[2].wait_recv()
    head_sum = zsend[2, pl.ds(0, 1), :] + zbuf[2, pl.ds(0, 1), :]

    slot = tp * 8 + dp
    mine = dbuf.at[slot]
    mine[pl.ds(0, 1), :] = sums_a[:, :LANES]
    mine[pl.ds(1, 1), :] = sums_a[:, LANES:]
    mine[pl.ds(2, 1), :] = sums_b[:, :LANES]
    mine[pl.ds(3, 1), :] = sums_b[:, LANES:2 * LANES]
    mine[pl.ds(4, 1), :] = jnp.concatenate([sums_b[:, 2 * LANES:], head_sum[:, :LANES // 2]], axis=1)
    pl.semaphore_wait(hx.at[2], 1)

    others = [(k, j) for k in (2, 1, 3, 0) for j in (4, 5, 2, 3, 6, 7, 1, 0) if (k, j) != (0, 0)]
    for k, j in others:
        pltpu.make_async_remote_copy(
            src_ref=mine, dst_ref=mine, send_sem=sums_sem.at[0], recv_sem=sums_sem.at[1],
            device_id=(rem(dp + j, 8), rem(tp + k, 4), cp), device_id_type=MESH).start()

    here = pl.ds(pl.multiple_of(core * (LANES // 2) + (TILES - 1) * LANES, LANES // 2), LANES)
    m_out[here, :] = moment(m_buf[here, :], m_out[here, :])
    step = jnp.full((1, LANES), steps[0], jnp.int32).astype(F32)
    keep_one = 1.0 - jnp.exp(step * math.log(BETA_ONE))
    keep_two = 1.0 - jnp.exp(step * math.log(BETA_TWO))
    n_out[...] = jnp.zeros(n_out.shape, F32)

    settled(snd_a, ss.at[0]).wait_send()
    settled(snd_b, ss.at[1]).wait_send()
    @pl.when(core == 1)
    def _():
        swap_extra.wait_send()

    settled(zsend, zs).wait_send()
    everyone_else = dbuf.at[pl.ds(0, len(others))]
    settled(everyone_else, sums_sem.at[0]).wait_send()
    settled(everyone_else, sums_sem.at[1]).wait_recv()

    def total(column):
        found = dbuf[column * 8]
        for p in range(1, 8):
            found = found + dbuf[column * 8 + p]
        return found

    whole = (total(0) + total(1)) + (total(2) + total(3))
    part = pltpu.roll(total(tp)[4:5, :], LANES // 2, 1)

    def advance(old, mean, n):
        new = BETA_TWO * old + (1.0 - BETA_TWO) * mean
        n_out[n:n + 1, :] = 1.0 / (keep_one * (jnp.sqrt(new / keep_two) + EPSILON))
        n_out[n + 8:n + 9, :] = new

    for k in range(5):
        if k < 4:
            old = dsec_v[pl.ds(k * LANES, LANES)].reshape(1, LANES)
        else:
            old = dsec_v[pl.ds(k * LANES, LANES // 2)].reshape(1, LANES // 2)
            old = jnp.concatenate([old, jnp.ones((1, LANES // 2), F32)], axis=1)
        advance(old, whole[k:k + 1, :] / FF, k)
    old = jnp.ones((1, LANES), F32)
    for h in range(4):
        old = jnp.where(lane == h, qsec_v[h], old)
    advance(old, part / (D * HEAD_DIM), 5)


def finish(
    n_in, m_in, qm_in, dp_in, qp_in,
    dp_out, dm_out, ds_out, du_out, qp_out, qm_out, qs_out, qu_out,
    po_buf, uo_buf, qpo, quo, ds_buf, qs_buf, out_sem,
):
    rows_d, width = dp_in.shape

    def store(n, src, dst):
        pltpu.make_async_copy(src, dst, out_sem.at[n]).start()

    def update(param, moment, scale):
        step = moment * scale
        param_new = param - LEARN_RATE * (step + DECAY_RATE * param)
        return param_new, step.astype(BF16)

    block = rows_d // 4
    store(0, m_in, dm_out)
    for k in range(5):
        count = LANES if k < 4 else width - 4 * LANES
        ds_buf[pl.ds(k * LANES, count)] = n_in[8 + k:9 + k, :count].reshape(count)
    qs_buf[...] = n_in[13:14, :4].reshape(4)
    store(1, ds_buf, ds_out)
    store(2, qs_buf, qs_out)
    for b in range(4):
        rows = pl.ds(b * block, block)
        for k in range(5):
            lanes = pl.ds(k * LANES, LANES if k < 4 else width - 4 * LANES)
            po_buf[rows, lanes], uo_buf[rows, lanes] = update(
                dp_in[rows, lanes], m_in[rows, lanes], n_in[k:k + 1, :lanes.size])
        store(3, po_buf.at[rows, :], dp_out.at[rows, :])
        store(4, uo_buf.at[rows, :], du_out.at[rows, :])
        if b == 0:
            store(5, qm_in, qm_out)
    for h in range(4):
        lanes = pl.ds(h * LANES, LANES)
        qpo[:, lanes], quo[:, lanes] = update(qp_in[:, lanes], qm_in[:, lanes], n_in[5:6, h:h + 1])
    store(6, qpo, qp_out)
    store(7, quo, qu_out)
    for n, (src, dst) in enumerate((
            (m_in, dm_out), (ds_buf, ds_out), (qs_buf, qs_out), (po_buf, dp_out), (uo_buf, du_out),
            (qm_in, qm_out), (qpo, qp_out), (quo, qu_out))):
        pltpu.make_async_copy(src, dst, out_sem.at[n]).wait()


def shards(nz, grad_down, grad_query, down_param, down_moment, down_second,
           query_param, query_moment, query_second, step_count):
    rows_d, width = down_param.shape
    rows_q, q_width = query_param.shape
    cut, wide = 2 * LANES, TILES * LANES
    rest, t_cols, q_half = width - cut, width, q_width // 2
    hbm = pl.BlockSpec(memory_space=pltpu.HBM)
    vmem = pl.BlockSpec(memory_space=pltpu.VMEM)
    dma = pltpu.SemaphoreType.DMA
    regular = pltpu.SemaphoreType.REGULAR
    grad_rows = jnp.swapaxes(grad_down, 1, 2)
    in_hbm = lambda x: pltpu.with_memory_space_constraint(x, pltpu.HBM)
    m, q_m, n = pl.pallas_call(
        functools.partial(exchange, nz),
        name="exchange",
        out_shape=(
            jax.ShapeDtypeStruct((rows_d, width), F32),
            jax.ShapeDtypeStruct((rows_q, q_width), F32),
            jax.ShapeDtypeStruct((16, LANES), F32),
        ),
        in_specs=[hbm, hbm, hbm, hbm, pl.BlockSpec(memory_space=pltpu.SMEM), hbm, hbm],
        out_specs=(vmem,) * 3,
        scratch_shapes=[
            pltpu.VMEM((4, width, wide), BF16),
            pltpu.VMEM((4, width, wide), BF16),
            pltpu.VMEM((4, rows_q, q_width), BF16),
            pltpu.VMEM((4, rows_q, q_width), BF16),
            pltpu.VMEM((3, TILES, cut, LANES), BF16),
            pltpu.VMEM((3, TILES, rest, LANES), BF16),
            pltpu.VMEM((2, 3, rows_q, q_half), BF16),
            pltpu.VMEM((TILES, cut, LANES), BF16),
            pltpu.VMEM((TILES, rest, LANES), BF16),
            pltpu.VMEM((2, rows_q, q_half), BF16),
            pltpu.VMEM((TILES, cut, LANES), BF16),
            pltpu.VMEM((TILES, rest, LANES), BF16),
            pltpu.VMEM((TILES, cut, LANES), BF16),
            pltpu.VMEM((TILES, rest, LANES), BF16),
            pltpu.VMEM((2, 2, rows_q, q_half), BF16),
            pltpu.VMEM((4, t_cols, LANES), BF16),
            pltpu.VMEM((4, t_cols, LANES), BF16),
            pltpu.VMEM((3, t_cols, LANES), BF16),
            pltpu.VMEM((t_cols, LANES), BF16),
            pltpu.VMEM((2, t_cols, LANES), BF16),
            pltpu.VMEM((TILES, width, LANES), F32),
            pltpu.VMEM((width, LANES), BF16),
            pltpu.VMEM((3, rows_q, q_width), BF16),
            pltpu.VMEM((width, LANES), F32),
            pltpu.VMEM((3, 8, LANES), F32),
            pltpu.VMEM((3, 8, LANES), F32),
            pltpu.VMEM((32, 5, LANES), F32),
            pltpu.VMEM((rows_d, width), F32),
            pltpu.VMEM((rows_q, q_width), F32),
            pltpu.VMEM((width,), F32),
            pltpu.SMEM((4,), F32),
            dma((4,)), dma((2,)), dma((10,)), dma((5,)), dma((10,)), dma((4,)), dma((2, TILES)), dma((1,)),
            dma, dma((3,)), dma((2,)), dma((4,)), dma((3,)),
            regular((3,)), regular((4,)), regular, regular((2,)), regular((2,)), dma((9,)),
        ],
        compiler_params=pltpu.CompilerParams(
            collective_id=0, has_side_effects=True, vmem_limit_bytes=28 << 20),
    )(in_hbm(grad_rows), in_hbm(grad_query), in_hbm(down_moment), in_hbm(query_moment), step_count,
      in_hbm(down_second), in_hbm(query_second))

    return tuple(pl.pallas_call(
        finish,
        name="finish",
        out_shape=(
            jax.ShapeDtypeStruct((rows_d, width), F32),
            jax.ShapeDtypeStruct((rows_d, width), F32),
            jax.ShapeDtypeStruct((width,), F32),
            jax.ShapeDtypeStruct((rows_d, width), BF16),
            jax.ShapeDtypeStruct((rows_q, q_width), F32),
            jax.ShapeDtypeStruct((rows_q, q_width), F32),
            jax.ShapeDtypeStruct((4,), F32),
            jax.ShapeDtypeStruct((rows_q, q_width), BF16),
        ),
        in_specs=[vmem] * 5,
        out_specs=(hbm,) * 8,
        scratch_shapes=[
            pltpu.VMEM((rows_d, width), F32),
            pltpu.VMEM((rows_d, width), BF16),
            pltpu.VMEM((rows_q, q_width), F32),
            pltpu.VMEM((rows_q, q_width), BF16),
            pltpu.VMEM((width,), F32),
            pltpu.VMEM((4,), F32),
            dma((8,)),
        ],
        compiler_params=pltpu.CompilerParams(vmem_limit_bytes=24 << 20),
    )(n, m, q_m, down_param, query_param))


def solution(mesh):
    in_specs = (
        P("dp", "tensor", "ctx"),
        P("dp", "ctx", "tensor"),
        P(("tensor", "dp"), "ctx"),
        P(("tensor", "dp"), "ctx"),
        P("ctx"),
        P(("ctx", "dp"), "tensor"),
        P(("ctx", "dp"), "tensor"),
        P("tensor"),
        P(),
    )
    out_specs = (
        P(("tensor", "dp"), "ctx"),
        P(("tensor", "dp"), "ctx"),
        P("ctx"),
        P(("tensor", "dp"), "ctx"),
        P(("ctx", "dp"), "tensor"),
        P(("ctx", "dp"), "tensor"),
        P("tensor"),
        P(("ctx", "dp"), "tensor"),
    )
    body = functools.partial(shards, mesh.shape["ctx"])
    return jax.shard_map(body, mesh=mesh, in_specs=in_specs, out_specs=out_specs, check_vma=False)
```
